32 devices in a mesh: groups: 2 (over y), frame: 4 (over z), space: 2 (over x), head: 2 (over core).
Axes of the slice: x: 2, y: 2, z: 4, core: 2. Of those that a mesh axis runs over, the one named last changes fastest.
Arguments:
- queries: bfloat16 [8, 512, 3072], P(('groups', 'frame'), 'space', 'head'), parts along dimension 0, may hold values from -6 to 6
- key_states: bfloat16 [8, 512, 3072], P(('groups', 'frame'), 'space', 'head'), parts along dimension 0, may hold values from -24 to 24
- value_states: bfloat16 [8, 512, 3072], P(('groups', 'frame'), 'space', 'head'), parts along dimension 0, may hold values from -6 to 6
- profile: int32 [24], replicated, may hold values from 0 to 1, as said below
- window: int32 [24], replicated, may hold values from 1 to 4, as said below
Outputs:
- attended: bfloat16 [8, 512, 3072], P(('groups', 'frame'), 'space', 'head'), parts along dimension 0
The draws below stay inside these ranges and needn't reach their ends.
There are 2 independent parts, one for each index of `groups`. The reference program is written for one: setup_inputs(seed, part) draws one part's arguments, and reference() takes and returns one part's arrays. A program takes and returns all parts, laid end to end along the dimension named above; an argument that names none is the same for every part. Nothing has to cross between parts.
Inputs may be any that keep to these rules, and one draw needn't show every extreme that they name: `profile`: 1 marks a head of frame-local attention, 0 a head of attention over a window of frames; exactly half of the 24 heads are marked 1. Some head marked 0 in profile has window 4.
All inputs are finite; a program needn't handle non-finite values.
Results may differ from the reference program's by a relative error of at most 0.0055.
Values may be sent and summed in bfloat16 or wider, within the bound.
A program may use at most 64 MiB of HBM per device.

```python
import jax
import jax.numpy as jnp
from jax import lax

H = 24
HD = 128
WMAX = 4
NTOK = 512
FRAMES = 4


def drawn_pair(key):
    base = jax.random.fold_in(key, 7)
    key_query, key_keys = jax.random.split(base, 2)
    shape_full = (FRAMES, NTOK, H * HD)
    query_draw = jnp.clip(jax.random.normal(key_query, shape_full, jnp.float32), -6.0, 6.0)
    key_draw = jnp.clip(jax.random.normal(key_keys, shape_full, jnp.float32), -6.0, 6.0)
    return (query_draw, key_draw)


def draw_queries(key, part):
    return drawn_pair(key)[0].astype(jnp.bfloat16)


def draw_key_states(key, part):
    return drawn_pair(key)[1].astype(jnp.bfloat16)


def head_classes(key):
    order = jax.random.permutation(jax.random.fold_in(key, 11), H)
    return (order < H // 2).astype(jnp.int32)


def draw_profile(key, part):
    return head_classes(key)


def draw_window(key, part):
    classes = head_classes(key)
    reaches = jax.random.randint(jax.random.fold_in(key, 13), (H,), 1, WMAX + 1)
    first_window = jnp.argmin(classes)
    return reaches.at[first_window].set(WMAX).astype(jnp.int32)


def level_of(rng, dims, cuts, low, high):
    def one(dim, parts):
        heights = jax.random.uniform(jax.random.fold_in(jax.random.fold_in(rng, 6), dim), (parts,), jnp.float32, low / len(cuts), high / len(cuts))
        return jnp.repeat(jnp.exp(heights), dims[dim] // parts).reshape((-1,) + (1,) * (len(dims) - dim - 1))

    loudness = one(*cuts[0])
    for cut in cuts[1:]:
        loudness = loudness * one(*cut)
    return loudness


def normal_values(key, shape, spread, bound, pieces=(), kind=jnp.bfloat16):
    drawn = jax.random.normal(key, shape, jnp.float32) * spread
    if len(pieces) > 0:
        drawn = level_of(key, shape, pieces, -0.22, 0.18) * drawn
    return jnp.clip(drawn, min=-bound, max=bound).astype(kind)


def setup_inputs(seed: int = 0, part: int = 0) -> dict:
    streams_of = jax.random.split(jax.random.key(seed), 6)
    part_splits = jax.random.split(jax.random.fold_in(streams_of[5], part), 6)
    return {
        "queries": draw_queries(jax.random.fold_in(jax.random.fold_in(streams_of[5], part), 71), part),
        "key_states": draw_key_states(jax.random.fold_in(jax.random.fold_in(streams_of[5], part), 71), part),
        "value_states": normal_values(part_splits[2], (FRAMES, NTOK, H * HD), 1.0, 6.0, ((0, 4), (1, 2), (2, 2))),
        "profile": draw_profile(jax.random.fold_in(streams_of[5], 71), part),
        "window": draw_window(jax.random.fold_in(streams_of[5], 71), part),
    }


def spatial_frames(queries, key_states, value_states):
    token_count = queries.shape[1]
    scale = HD ** -0.5

    def one_frame(item):
        query_frame, key_frame, value_frame = item
        query_heads = jnp.moveaxis(query_frame.reshape(token_count, H, HD), 1, 0)
        key_heads = jnp.moveaxis(key_frame.reshape(token_count, H, HD), 1, 0)
        value_heads = jnp.moveaxis(value_frame.reshape(token_count, H, HD), 1, 0)

        def one_head(triple):
            query_one, key_one, value_one = triple
            scores = jnp.dot(query_one, key_one.T, preferred_element_type=jnp.float32) * scale
            peak = jnp.max(scores, axis=1, keepdims=True)
            weights = jnp.exp(scores - peak)
            denominator = jnp.sum(weights, axis=1, keepdims=True)
            numerator = jnp.dot(weights.astype(jnp.bfloat16), value_one, preferred_element_type=jnp.float32)
            return numerator / denominator

        result = lax.map(one_head, (query_heads, key_heads, value_heads))
        return jnp.moveaxis(result, 0, 1)

    return lax.map(one_frame, (queries, key_states, value_states))


def temporal_frames(queries, key_states, value_states, window):
    frame_count, token_count = queries.shape[0], queries.shape[1]
    scale = HD ** -0.5
    shape_four = (frame_count, token_count, H, HD)
    query_heads = queries.reshape(shape_four).astype(jnp.float32)
    padding = ((WMAX, WMAX), (0, 0), (0, 0), (0, 0))
    key_padded = jnp.pad(key_states.reshape(shape_four), padding)
    value_padded = jnp.pad(value_states.reshape(shape_four), padding)
    frame_ids = jnp.arange(frame_count, dtype=jnp.int32)
    score_list = []
    for offset in range(-WMAX, WMAX + 1):
        near_keys = key_padded[WMAX + offset:WMAX + offset + frame_count]
        raw_scores = jnp.einsum("fnhd,fnhd->fnh", query_heads, near_keys.astype(jnp.float32)) * scale
        in_range = (frame_ids + offset >= 0) & (frame_ids + offset < frame_count)
        inside = in_range[:, None, None] & (window >= abs(offset))[None, None, :]
        score_list.append(jnp.where(inside, raw_scores, -1e30))
    scores = jnp.stack(score_list)
    peak = jnp.max(scores, axis=0)
    weights = jnp.exp(scores - peak[None])
    denominator = jnp.sum(weights, axis=0)
    rounded = weights.astype(jnp.bfloat16).astype(jnp.float32)
    numerator = jnp.zeros(shape_four, jnp.float32)
    for index, offset in enumerate(range(-WMAX, WMAX + 1)):
        near_values = value_padded[WMAX + offset:WMAX + offset + frame_count].astype(jnp.float32)
        numerator = numerator + rounded[index][..., None] * near_values
    return numerator / denominator[..., None]


def reference(queries, key_states, value_states, profile, window):
    spatial_part = spatial_frames(queries, key_states, value_states)
    temporal_part = temporal_frames(queries, key_states, value_states, window)
    chosen = jnp.where((profile == 1)[None, None, :, None], spatial_part, temporal_part)
    return chosen.reshape(queries.shape).astype(jnp.bfloat16)
```

```python
import functools

import jax
import jax.numpy as jnp
from jax import lax
from jax.experimental import pallas as pl
from jax.experimental.pallas import tpu as pltpu
from jax.sharding import PartitionSpec as P

HD = 128
WMAX = 4
SPREAD = 2
NEAR = 2
MESH = pl.DeviceIdType.MESH


def shared_kernel(
    frames, spaces, cores, prof_hbm, win_hbm, q_ref, k_ref, v_ref, out_ref,
    full, mine_first, theirs, squery, kv, tsend, trecv, tout, res,
    prof_ref, win_ref, pos, place, order, tab,
    loc_sem, d_send, d_recv, s_send, s_recv, t_send, t_recv, o_send, o_recv, r_send, r_recv,
):
    rows = q_ref.shape[1]
    here = q_ref.shape[2] // HD
    share = here // 2
    part = rows // frames
    scale = HD ** (-0.5)
    f = lax.axis_index("frame")
    x = lax.axis_index("space")
    c = lax.axis_index("head")
    others_f = [lax.rem(f + d, frames) for d in range(1, frames)]
    others_x = [lax.rem(x + d, spaces) for d in range(1, spaces)]
    others_c = [lax.rem(c + d, cores) for d in range(1, cores)]
    side = f // (frames // 2)
    far_first = [
        lax.rem(f + (1 - side) * (frames - 1 - i) + side * (1 + i), frames)
        for i in range(frames - 1)
    ]

    def remote(src, dst, send, recv, **target):
        return pltpu.make_async_remote_copy(
            src_ref=src, dst_ref=dst, send_sem=send, recv_sem=recv,
            device_id=target, device_id_type=MESH,
        )

    def lanes(h):
        return pl.ds(pl.multiple_of(h * HD, HD), HD)

    small = (
        pltpu.make_async_copy(prof_hbm, prof_ref, loc_sem.at[3]),
        pltpu.make_async_copy(win_hbm, win_ref, loc_sem.at[4]),
    )
    for copy in small:
        copy.start()
    sources = (k_ref, v_ref, q_ref)
    for n, src in enumerate(sources):
        def local_start(h, _):
            pltpu.make_async_copy(src.at[0, :, lanes(h)], full.at[n, h], loc_sem.at[n]).start()
            return 0

        lax.fori_loop(0, here, local_start, 0)

    barrier = pltpu.get_barrier_semaphore()
    for other in others_c:
        pl.semaphore_signal(barrier, inc=1, device_id={"head": other}, device_id_type=MESH)
    for other in others_x:
        pl.semaphore_signal(barrier, inc=1, device_id={"space": other}, device_id_type=MESH)
    for other in others_f:
        pl.semaphore_signal(barrier, inc=1, device_id={"frame": other}, device_id_type=MESH)

    for copy in small:
        copy.wait()

    count = jnp.int32(0)
    for h in range(here):
        count = count + prof_ref[h]
    first_space = (count >= share).astype(jnp.int32)
    main_count = jnp.maximum(count, here - count)
    for e in range(cores):
        main = first_space if e == 0 else 1 - first_space
        major = jnp.int32(0)
        minor = main_count
        for h in range(here):
            p = prof_ref[e * here + h]
            is_main = p * main + (1 - p) * (1 - main)
            slot = jnp.clip(is_main * major + (1 - is_main) * minor, 0, here - 1)
            major = major + is_main
            minor = minor + (1 - is_main)
            away = ((slot >= share) & (slot < main_count)).astype(jnp.int32)
            owner = away * (1 - e) + (1 - away) * e
            pos[e * here + h] = slot
            place[e * here + h] = owner * here + (1 - p) * share + slot - (slot >= share).astype(jnp.int32) * share

    def fill(slot, _):
        head = jnp.int32(0)
        for h in range(here):
            head = head + jnp.where(pos[c * here + h] == slot, h, 0)
        order[slot] = jnp.clip(head, 0, here - 1)
        return 0

    lax.fori_loop(0, here, fill, 0)

    for n in range(3):
        pltpu.make_async_copy(full.at[n], full.at[n], loc_sem.at[n]).wait()

    def arrange(slot, _):
        head = order[slot]
        for n in range(3):
            mine_first[slot, n] = full[n, head]
        return 0

    lax.fori_loop(0, here, arrange, 0)

    pl.semaphore_wait(barrier, len(others_c) + len(others_x) + len(others_f))

    partner = others_c[0]

    def core_copy(j):
        return remote(mine_first.at[share + j], theirs.at[j], d_send.at[j], d_recv.at[j], head=partner)

    def core_start(j, _):
        core_copy(j).start()
        return 0

    lax.fori_loop(0, share, core_start, 0)

    main_space = c * (1 - first_space) + (1 - c) * first_space
    my_rows = pl.ds(pl.multiple_of(x * rows, rows), rows)
    mine = pl.ds(pl.multiple_of(f * part, part), part)

    def window_copy(j, other):
        return remote(
            tsend.at[j, other], trecv.at[f, j], t_send.at[other, j], t_recv.at[f, j], frame=other
        )

    def space_copy(j, other):
        return remote(
            kv.at[j, :, my_rows], kv.at[j, :, my_rows], s_send.at[other, j], s_recv.at[x, j], space=other
        )

    def gather(j, _):
        core_copy(j).wait_recv()
        borrowed = share + j < main_count
        for n in range(3):
            head_main = mine_first[j, n]
            head_rest = jnp.where(borrowed, theirs[j, n], mine_first[share + j, n])
            block = jnp.where(main_space == 1, head_rest, head_main)
            for g in range(frames):
                tsend[j, g, n] = block[g * part:(g + 1) * part]
            block = jnp.where(main_space == 1, head_main, head_rest)
            if n < 2:
                kv[j, n, my_rows] = block
            else:
                squery[j] = block
        for other in far_first:
            window_copy(j, other).start()

        @pl.when(j > 0)
        def _():
            for other in others_x:
                space_copy(j - 1, other).start()

        return 0

    lax.fori_loop(0, share, gather, 0)

    def fill_reach(j, _):
        own_slot = j + main_space * share
        far = ((main_space == 1) & (share + j < main_count)).astype(jnp.int32)
        own_reach = jnp.int32(0)
        far_reach = jnp.int32(0)
        for h in range(here):
            own_reach = own_reach + jnp.where(pos[c * here + h] == own_slot, win_ref[c * here + h], 0)
            far_reach = far_reach + jnp.where(
                pos[partner * here + h] == share + j, win_ref[partner * here + h], 0
            )
        tab[j] = far * far_reach + (1 - far) * own_reach
        return 0

    lax.fori_loop(0, share, fill_reach, 0)

    def out_copy(j, other):
        return remote(
            tout.at[j, other], res.at[c * here + share + j, mine], o_send.at[other, j], o_recv.at[f, j], frame=other
        )

    def back_copy(slot, other):
        return remote(
            res.at[c * here + slot], res.at[c * here + slot], r_send.at[other, slot], r_recv.at[c, slot], head=other
        )

    for other in others_x:
        space_copy(share - 1, other).start()

    def step(j, _):
        for other in others_f:
            remote(
                tsend.at[j, other], trecv.at[other, j], t_send.at[other, j], t_recv.at[other, j], frame=other
            ).wait_recv()
        trecv[f, j] = tsend[j, f]
        reach = tab[j]
        qs = [trecv[g, j, 2].astype(jnp.float32) for g in range(frames)]
        ks = [trecv[g, j, 0].astype(jnp.float32) for g in range(frames)]
        vs = [trecv[g, j, 1].astype(jnp.float32) for g in range(frames)]
        for g in range(frames):
            near = [m for m in range(frames) if abs(m - g) <= WMAX]
            scores = []
            for m in near:
                raw = jnp.sum(qs[g] * ks[m], axis=-1, keepdims=True) * scale
                scores.append(jnp.where(reach >= abs(m - g), raw, -1e30))
            peak = functools.reduce(jnp.maximum, scores)
            weights = [jnp.exp(s - peak) for s in scores]
            total = functools.reduce(jnp.add, weights)
            acc = functools.reduce(
                jnp.add,
                [w.astype(jnp.bfloat16).astype(jnp.float32) * vs[m] for w, m in zip(weights, near)],
            )
            tout[j, g] = (acc / total).astype(jnp.bfloat16)
        res[c * here + share + j, mine] = tout[j, f]

        for other in others_x:
            other_rows = pl.ds(pl.multiple_of(other * rows, rows), rows)
            remote(
                kv.at[j, :, other_rows], kv.at[j, :, other_rows],
                s_send.at[other, j], s_recv.at[other, j], space=other,
            ).wait_recv()
        query = squery[j]
        scores = lax.dot_general(
            query, kv[j, 0], (((1,), (1,)), ((), ())), preferred_element_type=jnp.float32
        ) * scale
        peak = jnp.max(scores, axis=1, keepdims=True)
        weights = jnp.exp(scores - peak)
        total = jnp.sum(weights, axis=1, keepdims=True)
        acc = jnp.dot(weights.astype(jnp.bfloat16), kv[j, 1], preferred_element_type=jnp.float32)
        res[c * here + j] = (acc / total).astype(jnp.bfloat16)

        for other in far_first:
            out_copy(j, other).start()

        @pl.when(j > 0)
        def _():
            for other in others_c:
                back_copy(j - 1, other).start()

        return 0

    lax.fori_loop(0, share, step, 0)
    for other in others_c:
        back_copy(share - 1, other).start()

    def forward(j, _):
        for other in others_f:
            theirs = pl.ds(pl.multiple_of(other * part, part), part)
            remote(
                tout.at[j, other], res.at[c * here + share + j, theirs], o_send.at[other, j], o_recv.at[other, j],
                frame=other,
            ).wait_recv()
        for other in others_c:
            back_copy(share + j, other).start()
        return 0

    lax.fori_loop(0, share, forward, 0)

    def arrive(slot, _):
        for other in others_c:
            remote(
                res.at[c * here + slot], res.at[other * here + slot], r_send.at[other, slot], r_recv.at[other, slot], head=other
            ).wait_recv()
        return 0

    lax.fori_loop(0, 2 * share, arrive, 0)

    for i in range(here):
        out_ref[0, :, i * HD:(i + 1) * HD] = res[place[c * here + i]]


    def drain(j, _):
        core_copy(j).wait_send()
        for other in others_f:
            window_copy(j, other).wait_send()
            out_copy(j, other).wait_send()
        for other in others_x:
            space_copy(j, other).wait_send()
        for other in others_c:
            back_copy(j, other).wait_send()
            back_copy(share + j, other).wait_send()
        return 0

    lax.fori_loop(0, share, drain, 0)


def direct_kernel(
    frames, spaces, cores, fulls, nears, prof_hbm, win_hbm, q_ref, k_ref, v_ref, out_ref,
    full, kv, tsend, trecv, tout, res, nsend, nrecv,
    prof_ref, win_ref, pos, order,
    loc_sem, s_send, s_recv, t_send, t_recv, o_send, o_recv, n_send, n_recv,
):
    rows = q_ref.shape[1]
    here = q_ref.shape[2] // HD
    part = rows // frames
    scale = HD ** (-0.5)
    f = lax.axis_index("frame")
    x = lax.axis_index("space")
    c = lax.axis_index("head")
    others_f = [lax.rem(f + d, frames) for d in range(1, frames)]
    others_x = [lax.rem(x + d, spaces) for d in range(1, spaces)]
    side = f // (frames // 2)
    far_first = [
        lax.rem(f + (1 - side) * (frames - 1 - i) + side * (1 + i), frames)
        for i in range(frames - 1)
    ]

    def of_core(counts):
        total = jnp.int32(counts[0])
        for e in range(1, cores):
            total = jnp.where(c == e, jnp.int32(counts[e]), total)
        return total

    n_full = of_core(fulls)
    n_near = of_core(nears)
    n_time = n_full + n_near
    n_space = here - n_time

    def remote(src, dst, send, recv, **target):
        return pltpu.make_async_remote_copy(
            src_ref=src, dst_ref=dst, send_sem=send, recv_sem=recv,
            device_id=target, device_id_type=MESH,
        )

    def lanes(h):
        return pl.ds(pl.multiple_of(h * HD, HD), HD)

    small = (
        pltpu.make_async_copy(prof_hbm, prof_ref, loc_sem.at[3]),
        pltpu.make_async_copy(win_hbm, win_ref, loc_sem.at[4]),
    )
    for copy in small:
        copy.start()

    barrier = pltpu.get_barrier_semaphore()
    for other in others_x:
        pl.semaphore_signal(barrier, inc=1, device_id={"space": other}, device_id_type=MESH)
    for other in others_f:
        pl.semaphore_signal(barrier, inc=1, device_id={"frame": other}, device_id_type=MESH)

    for n, src in enumerate((k_ref, v_ref, q_ref)):
        def local_start(h, _):
            pltpu.make_async_copy(src.at[0, :, lanes(h)], full.at[n, h], loc_sem.at[n]).start()
            return 0

        lax.fori_loop(0, here, local_start, 0)

    for copy in small:
        copy.wait()

    def class_of(h):
        p = prof_ref[c * here + h]
        one = (win_ref[c * here + h] == 1).astype(jnp.int32)
        return p * 2 + (1 - p) * one

    kinds = [class_of(h) for h in range(here)]
    tops = []
    start = jnp.int32(0)
    for kind in range(3):
        tops.append(start)
        for h in range(here):
            start = start + (kinds[h] == kind).astype(jnp.int32)
    for h in range(here):
        slot = jnp.int32(0)
        for kind in range(3):
            is_kind = kinds[h] == kind
            slot = jnp.where(is_kind, tops[kind], slot)
            tops[kind] = tops[kind] + is_kind.astype(jnp.int32)
        pos[h] = jnp.clip(slot, 0, here - 1)

    def fill(slot, _):
        head = jnp.int32(0)
        for h in range(here):
            head = head + jnp.where(pos[h] == slot, h, 0)
        order[slot] = jnp.clip(head, 0, here - 1)
        return 0

    lax.fori_loop(0, here, fill, 0)

    for n in range(3):
        pltpu.make_async_copy(full.at[n], full.at[n], loc_sem.at[n]).wait()

    pl.semaphore_wait(barrier, len(others_x) + len(others_f))

    my_rows = pl.ds(pl.multiple_of(x * rows, rows), rows)
    mine = pl.ds(pl.multiple_of(f * part, part), part)

    def window_copy(j, other):
        return remote(
            tsend.at[j, other], trecv.at[f, j], t_send.at[other, j], t_recv.at[f, j], frame=other
        )

    def window_arrival(j, other):
        return remote(
            tsend.at[j, other], trecv.at[other, j], t_send.at[other, j], t_recv.at[other, j], frame=other
        )

    def space_copy(j, other):
        return remote(
            kv.at[j, :, my_rows], kv.at[j, :, my_rows], s_send.at[other, j], s_recv.at[x, j], space=other
        )

    def space_arrival(j, other):
        other_rows = pl.ds(pl.multiple_of(other * rows, rows), rows)
        return remote(
            kv.at[j, :, other_rows], kv.at[j, :, other_rows], s_send.at[other, j], s_recv.at[other, j], space=other
        )

    def out_copy(j, other):
        return remote(
            tout.at[j, other], res.at[j, mine], o_send.at[other, j], o_recv.at[f, j], frame=other
        )

    def out_arrival(j, other):
        rows_there = pl.ds(pl.multiple_of(other * part, part), part)
        return remote(
            tout.at[j, other], res.at[j, rows_there], o_send.at[other, j], o_recv.at[other, j], frame=other
        )

    def near_copy(j, up):
        return remote(
            nsend.at[j], nrecv.at[1 - up, j], n_send.at[up, j], n_recv.at[1 - up, j],
            frame=jnp.clip(f + 2 * up - 1, 0, frames - 1),
        )

    def near_arrival(j, above):
        return remote(
            nsend.at[j], nrecv.at[above, j], n_send.at[above, j], n_recv.at[above, j],
            frame=jnp.clip(f + 2 * above - 1, 0, frames - 1),
        )

    has = (f > 0, f < frames - 1)

    def prepare(j, _):
        @pl.when(j < n_full)
        def _():
            head = order[j]
            for n in range(3):
                block = full[n, head]
                for g in range(frames):
                    tsend[j, g, n] = block[g * part:(g + 1) * part]
            for other in far_first:
                window_copy(j, other).start()

        @pl.when(j < n_space)
        def _():
            head = order[n_time + j]
            for n in range(2):
                kv[j, n, my_rows] = full[n, head]
            for other in others_x:
                space_copy(j, other).start()

        return 0

    lax.fori_loop(0, here, prepare, 0)

    def prepare_near(j, _):
        head = order[n_full + j]
        for n in range(2):
            nsend[j, n] = full[n, head]
        for up in range(2):
            @pl.when(has[up])
            def _():
                near_copy(j, up).start()

        return 0

    if max(nears) > 0:
        lax.fori_loop(0, n_near, prepare_near, 0)

    def step(j, _):
        @pl.when(j < n_full)
        def _():
            for other in others_f:
                window_arrival(j, other).wait_recv()
            trecv[f, j] = tsend[j, f]
            reach = win_ref[c * here + order[j]]
            qs = [trecv[g, j, 2].astype(jnp.float32) for g in range(frames)]
            ks = [trecv[g, j, 0].astype(jnp.float32) for g in range(frames)]
            vs = [trecv[g, j, 1].astype(jnp.float32) for g in range(frames)]
            for g in range(frames):
                close = [m for m in range(frames) if abs(m - g) <= WMAX]
                scores = []
                for m in close:
                    raw = jnp.sum(qs[g] * ks[m], axis=-1, keepdims=True) * scale
                    scores.append(jnp.where(reach >= abs(m - g), raw, -1e30))
                peak = functools.reduce(jnp.maximum, scores)
                weights = [jnp.exp(s - peak) for s in scores]
                total = functools.reduce(jnp.add, weights)
                acc = functools.reduce(
                    jnp.add,
                    [w.astype(jnp.bfloat16).astype(jnp.float32) * vs[m] for w, m in zip(weights, close)],
                )
                tout[j, g] = (acc / total).astype(jnp.bfloat16)
            res[j, mine] = tout[j, f]
            for other in far_first:
                out_copy(j, other).start()

        @pl.when(j < n_space)
        def _():
            for other in others_x:
                space_arrival(j, other).wait_recv()
            query = full[2, order[n_time + j]]
            scores = lax.dot_general(
                query, kv[j, 0], (((1,), (1,)), ((), ())), preferred_element_type=jnp.float32
            ) * scale
            peak = jnp.max(scores, axis=1, keepdims=True)
            weights = jnp.exp(scores - peak)
            total = jnp.sum(weights, axis=1, keepdims=True)
            acc = jnp.dot(weights.astype(jnp.bfloat16), kv[j, 1], preferred_element_type=jnp.float32)
            res[n_time + j] = (acc / total).astype(jnp.bfloat16)

        return 0

    lax.fori_loop(0, here, step, 0)

    chunk = min(rows, 64)

    def near_step(j, _):
        for above in range(2):
            @pl.when(has[above])
            def _():
                near_arrival(j, above).wait_recv()

            @pl.when(jnp.logical_not(has[above]))
            def _():
                nrecv[above, j] = nsend[j]

        head = order[n_full + j]

        def rows_step(i, _):
            at = pl.ds(pl.multiple_of(i * chunk, chunk), chunk)
            query = full[2, head, at].astype(jnp.float32)
            keys = (nrecv[0, j, 0, at], nsend[j, 0, at], nrecv[1, j, 0, at])
            values = (nrecv[0, j, 1, at], nsend[j, 1, at], nrecv[1, j, 1, at])
            takes = (has[0], None, has[1])
            scores = []
            for key, take in zip(keys, takes):
                raw = jnp.sum(query * key.astype(jnp.float32), axis=-1, keepdims=True) * scale
                scores.append(raw if take is None else jnp.where(take, raw, -1e30))
            peak = functools.reduce(jnp.maximum, scores)
            weights = [jnp.exp(s - peak) for s in scores]
            total = functools.reduce(jnp.add, weights)
            acc = functools.reduce(
                jnp.add,
                [w.astype(jnp.bfloat16).astype(jnp.float32) * v.astype(jnp.float32) for w, v in zip(weights, values)],
            )
            res[n_full + j, at] = (acc / total).astype(jnp.bfloat16)
            return 0

        lax.fori_loop(0, rows // chunk, rows_step, 0)
        return 0

    if max(nears) > 0:
        lax.fori_loop(0, n_near, near_step, 0)

    def arrive(j, _):
        for other in others_f:
            out_arrival(j, other).wait_recv()
        return 0

    lax.fori_loop(0, n_full, arrive, 0)

    for i in range(here):
        out_ref[0, :, i * HD:(i + 1) * HD] = res[pos[i]]

    def drain_full(j, _):
        for other in others_f:
            window_copy(j, other).wait_send()
            out_copy(j, other).wait_send()
        return 0

    def drain_space(j, _):
        for other in others_x:
            space_copy(j, other).wait_send()
        return 0

    def drain_near(j, _):
        for up in range(2):
            @pl.when(has[up])
            def _():
                near_copy(j, up).wait_send()

        return 0

    lax.fori_loop(0, n_full, drain_full, 0)
    lax.fori_loop(0, n_space, drain_space, 0)
    if max(nears) > 0:
        lax.fori_loop(0, n_near, drain_near, 0)


def direct(sizes, times, nears, number, queries, key_states, value_states, profile, window):
    frames, spaces, cores = sizes
    rows = queries.shape[1]
    here = queries.shape[2] // HD
    part = rows // frames
    fulls = tuple(t - n for t, n in zip(times, nears))
    most_full, most_near = max(1, *fulls), max(1, *nears)
    most_space = max(1, *(here - t for t in times))
    bf = jnp.bfloat16
    dma = pltpu.SemaphoreType.DMA
    return pl.pallas_call(
        functools.partial(direct_kernel, frames, spaces, cores, fulls, nears),
        out_shape=pltpu.VMEM(queries.shape, queries.dtype),
        in_specs=[pl.BlockSpec(memory_space=pltpu.HBM)] * 5,
        out_specs=pl.BlockSpec(memory_space=pltpu.VMEM),
        scratch_shapes=[
            pltpu.VMEM((3, here, rows, HD), bf),
            pltpu.VMEM((most_space, 2, spaces * rows, HD), bf),
            pltpu.VMEM((most_full, frames, 3, part, HD), bf),
            pltpu.VMEM((frames, most_full, 3, part, HD), bf),
            pltpu.VMEM((most_full, frames, part, HD), bf),
            pltpu.VMEM((here, rows, HD), bf),
            pltpu.VMEM((most_near, 2, rows, HD), bf),
            pltpu.VMEM((2, most_near, 2, rows, HD), bf),
            pltpu.SMEM((here * cores,), jnp.int32),
            pltpu.SMEM((here * cores,), jnp.int32),
            pltpu.SMEM((here,), jnp.int32),
            pltpu.SMEM((here,), jnp.int32),
            dma((5,)),
            dma((spaces, most_space)),
            dma((spaces, most_space)),
            dma((frames, most_full)),
            dma((frames, most_full)),
            dma((frames, most_full)),
            dma((frames, most_full)),
            dma((2, most_near)),
            dma((2, most_near)),
        ],
        compiler_params=pltpu.CompilerParams(
            collective_id=number, has_side_effects=True, vmem_limit_bytes=60 * 1024 * 1024
        ),
    )(profile, window, queries, key_states, value_states)


def shared(sizes, queries, key_states, value_states, profile, window):
    frames, spaces, cores = sizes
    rows = queries.shape[1]
    here = queries.shape[2] // HD
    share = here // 2
    part = rows // frames
    any_space = pl.BlockSpec(memory_space=pltpu.HBM)
    bf = jnp.bfloat16
    dma = pltpu.SemaphoreType.DMA
    return pl.pallas_call(
        functools.partial(shared_kernel, frames, spaces, cores),
        out_shape=pltpu.VMEM(queries.shape, queries.dtype),
        in_specs=[any_space] * 5,
        out_specs=pl.BlockSpec(memory_space=pltpu.VMEM),
        scratch_shapes=[
            pltpu.VMEM((3, here, rows, HD), bf),
            pltpu.VMEM((here, 3, rows, HD), bf),
            pltpu.VMEM((share, 3, rows, HD), bf),
            pltpu.VMEM((share, rows, HD), bf),
            pltpu.VMEM((share, 2, spaces * rows, HD), bf),
            pltpu.VMEM((share, frames, 3, part, HD), bf),
            pltpu.VMEM((frames, share, 3, part, HD), bf),
            pltpu.VMEM((share, frames, part, HD), bf),
            pltpu.VMEM((cores * 2 * share, rows, HD), bf),
            pltpu.SMEM((here * cores,), jnp.int32),
            pltpu.SMEM((here * cores,), jnp.int32),
            pltpu.SMEM((here * cores,), jnp.int32),
            pltpu.SMEM((here * cores,), jnp.int32),
            pltpu.SMEM((here,), jnp.int32),
            pltpu.SMEM((share,), jnp.int32),
            dma((5,)),
            dma((share,)),
            dma((share,)),
            dma((spaces, share)),
            dma((spaces, share)),
            dma((frames, share)),
            dma((frames, share)),
            dma((frames, share)),
            dma((frames, share)),
            dma((cores, 2 * share)),
            dma((cores, 2 * share)),
        ],
        compiler_params=pltpu.CompilerParams(
            collective_id=0, has_side_effects=True, vmem_limit_bytes=60 * 1024 * 1024
        ),
    )(profile, window, queries, key_states, value_states)


def choose_kernel(cores, spans, most_near, prof_ref, win_ref, out_ref):
    here = prof_ref.shape[0] // cores
    fewest = jnp.int32(most_near)
    first = jnp.int32(0)
    for e in range(cores):
        near = jnp.int32(0)
        for h in range(here):
            timed = 1 - prof_ref[e * here + h]
            if e == 0:
                first = first + timed
            near = near + timed * (win_ref[e * here + h] == 1).astype(jnp.int32)
        fewest = jnp.minimum(fewest, near)
    low, high = spans
    index = (first - low) * (most_near + 1) + fewest + 1
    out_ref[0] = jnp.where((first >= low) & (first <= high), index, 0)


def local(sizes, queries, key_states, value_states, profile, window):
    frames, spaces, cores = sizes
    here = queries.shape[2] // HD
    low, high = here // 2 - SPREAD, here // 2 + SPREAD
    smem = pl.BlockSpec(memory_space=pltpu.SMEM)
    index = pl.pallas_call(
        functools.partial(choose_kernel, cores, (low, high), NEAR),
        out_shape=jax.ShapeDtypeStruct((1,), jnp.int32),
        in_specs=[smem, smem],
        out_specs=smem,
    )(profile, window)
    ways = [functools.partial(shared, sizes)]
    for first in range(low, high + 1):
        for near in range(NEAR + 1):
            ways.append(functools.partial(direct, sizes, (first, here - first), (near, near), len(ways)))
    return lax.switch(index[0], ways, queries, key_states, value_states, profile, window)


def solution(mesh):
    spec = P(("groups", "frame"), "space", "head")
    sizes = (mesh.shape["frame"], mesh.shape["space"], mesh.shape["head"])
    return jax.shard_map(
        functools.partial(local, sizes),
        mesh=mesh,
        in_specs=(spec, spec, spec, P(), P()),
        out_specs=spec,
        check_vma=False,
    )
```

```python
import functools
import itertools

import jax
import jax.numpy as jnp
from jax import lax
from jax.experimental import pallas as pl
from jax.experimental.pallas import tpu as pltpu
from jax.sharding import PartitionSpec as P

HD = 128
WMAX = 4
CAPS = {0: 2, -1: 2, 1: 2, -2: 1, 2: 1}
EARLY = 2
MESH = pl.DeviceIdType.MESH


def shared_kernel(
    frames, spaces, cores, prof_hbm, win_hbm, q_ref, k_ref, v_ref, out_ref,
    full, mine_first, theirs, squery, kv, tsend, trecv, tout, res,
    prof_ref, win_ref, pos, place, order, tab,
    loc_sem, d_send, d_recv, s_send, s_recv, t_send, t_recv, o_send, o_recv, r_send, r_recv,
):
    rows = q_ref.shape[1]
    here = q_ref.shape[2] // HD
    share = here // 2
    part = rows // frames
    scale = HD ** (-0.5)
    f = lax.axis_index("frame")
    x = lax.axis_index("space")
    c = lax.axis_index("head")
    others_f = [lax.rem(f + d, frames) for d in range(1, frames)]
    others_x = [lax.rem(x + d, spaces) for d in range(1, spaces)]
    others_c = [lax.rem(c + d, cores) for d in range(1, cores)]
    side = f // (frames // 2)
    far_first = [
        lax.rem(f + (1 - side) * (frames - 1 - i) + side * (1 + i), frames)
        for i in range(frames - 1)
    ]

    def remote(src, dst, send, recv, **target):
        return pltpu.make_async_remote_copy(
            src_ref=src, dst_ref=dst, send_sem=send, recv_sem=recv,
            device_id=target, device_id_type=MESH,
        )

    def lanes(h):
        return pl.ds(pl.multiple_of(h * HD, HD), HD)

    small = (
        pltpu.make_async_copy(prof_hbm, prof_ref, loc_sem.at[3]),
        pltpu.make_async_copy(win_hbm, win_ref, loc_sem.at[4]),
    )
    for copy in small:
        copy.start()
    sources = (k_ref, v_ref, q_ref)
    for n, src in enumerate(sources):
        def local_start(h, _):
            pltpu.make_async_copy(src.at[0, :, lanes(h)], full.at[n, h], loc_sem.at[n]).start()
            return 0

        lax.fori_loop(0, here, local_start, 0)

    barrier = pltpu.get_barrier_semaphore()
    for other in others_c:
        pl.semaphore_signal(barrier, inc=1, device_id={"head": other}, device_id_type=MESH)
    for other in others_x:
        pl.semaphore_signal(barrier, inc=1, device_id={"space": other}, device_id_type=MESH)
    for other in others_f:
        pl.semaphore_signal(barrier, inc=1, device_id={"frame": other}, device_id_type=MESH)

    for copy in small:
        copy.wait()

    count = jnp.int32(0)
    for h in range(here):
        count = count + prof_ref[h]
    first_space = (count >= share).astype(jnp.int32)
    main_count = jnp.maximum(count, here - count)
    for e in range(cores):
        main = first_space if e == 0 else 1 - first_space
        major = jnp.int32(0)
        minor = main_count
        for h in range(here):
            p = prof_ref[e * here + h]
            is_main = p * main + (1 - p) * (1 - main)
            slot = jnp.clip(is_main * major + (1 - is_main) * minor, 0, here - 1)
            major = major + is_main
            minor = minor + (1 - is_main)
            away = ((slot >= share) & (slot < main_count)).astype(jnp.int32)
            owner = away * (1 - e) + (1 - away) * e
            pos[e * here + h] = slot
            place[e * here + h] = owner * here + (1 - p) * share + slot - (slot >= share).astype(jnp.int32) * share

    def fill(slot, _):
        head = jnp.int32(0)
        for h in range(here):
            head = head + jnp.where(pos[c * here + h] == slot, h, 0)
        order[slot] = jnp.clip(head, 0, here - 1)
        return 0

    lax.fori_loop(0, here, fill, 0)

    for n in range(3):
        pltpu.make_async_copy(full.at[n], full.at[n], loc_sem.at[n]).wait()

    def arrange(slot, _):
        head = order[slot]
        for n in range(3):
            mine_first[slot, n] = full[n, head]
        return 0

    lax.fori_loop(0, here, arrange, 0)

    pl.semaphore_wait(barrier, len(others_c) + len(others_x) + len(others_f))

    partner = others_c[0]

    def core_copy(j):
        return remote(mine_first.at[share + j], theirs.at[j], d_send.at[j], d_recv.at[j], head=partner)

    def core_start(j, _):
        core_copy(j).start()
        return 0

    lax.fori_loop(0, share, core_start, 0)

    main_space = c * (1 - first_space) + (1 - c) * first_space
    my_rows = pl.ds(pl.multiple_of(x * rows, rows), rows)
    mine = pl.ds(pl.multiple_of(f * part, part), part)

    def window_copy(j, other):
        return remote(
            tsend.at[j, other], trecv.at[f, j], t_send.at[other, j], t_recv.at[f, j], frame=other
        )

    def space_copy(j, other):
        return remote(
            kv.at[j, :, my_rows], kv.at[j, :, my_rows], s_send.at[other, j], s_recv.at[x, j], space=other
        )

    def gather(j, _):
        core_copy(j).wait_recv()
        borrowed = share + j < main_count
        for n in range(3):
            head_main = mine_first[j, n]
            head_rest = jnp.where(borrowed, theirs[j, n], mine_first[share + j, n])
            block = jnp.where(main_space == 1, head_rest, head_main)
            for g in range(frames):
                tsend[j, g, n] = block[g * part:(g + 1) * part]
            block = jnp.where(main_space == 1, head_main, head_rest)
            if n < 2:
                kv[j, n, my_rows] = block
            else:
                squery[j] = block
        for other in far_first:
            window_copy(j, other).start()

        @pl.when(j > 0)
        def _():
            for other in others_x:
                space_copy(j - 1, other).start()

        return 0

    lax.fori_loop(0, share, gather, 0)

    def fill_reach(j, _):
        own_slot = j + main_space * share
        far = ((main_space == 1) & (share + j < main_count)).astype(jnp.int32)
        own_reach = jnp.int32(0)
        far_reach = jnp.int32(0)
        for h in range(here):
            own_reach = own_reach + jnp.where(pos[c * here + h] == own_slot, win_ref[c * here + h], 0)
            far_reach = far_reach + jnp.where(
                pos[partner * here + h] == share + j, win_ref[partner * here + h], 0
            )
        tab[j] = far * far_reach + (1 - far) * own_reach
        return 0

    lax.fori_loop(0, share, fill_reach, 0)

    def out_copy(j, other):
        return remote(
            tout.at[j, other], res.at[c * here + share + j, mine], o_send.at[other, j], o_recv.at[f, j], frame=other
        )

    def back_copy(slot, other):
        return remote(
            res.at[c * here + slot], res.at[c * here + slot], r_send.at[other, slot], r_recv.at[c, slot], head=other
        )

    for other in others_x:
        space_copy(share - 1, other).start()

    def step(j, _):
        for other in others_f:
            remote(
                tsend.at[j, other], trecv.at[other, j], t_send.at[other, j], t_recv.at[other, j], frame=other
            ).wait_recv()
        trecv[f, j] = tsend[j, f]
        reach = tab[j]
        qs = [trecv[g, j, 2].astype(jnp.float32) for g in range(frames)]
        ks = [trecv[g, j, 0].astype(jnp.float32) for g in range(frames)]
        vs = [trecv[g, j, 1].astype(jnp.float32) for g in range(frames)]
        for g in range(frames):
            near = [m for m in range(frames) if abs(m - g) <= WMAX]
            scores = []
            for m in near:
                raw = jnp.sum(qs[g] * ks[m], axis=-1, keepdims=True) * scale
                scores.append(jnp.where(reach >= abs(m - g), raw, -1e30))
            peak = functools.reduce(jnp.maximum, scores)
            weights = [jnp.exp(s - peak) for s in scores]
            total = functools.reduce(jnp.add, weights)
            acc = functools.reduce(
                jnp.add,
                [w.astype(jnp.bfloat16).astype(jnp.float32) * vs[m] for w, m in zip(weights, near)],
            )
            tout[j, g] = (acc / total).astype(jnp.bfloat16)
        res[c * here + share + j, mine] = tout[j, f]

        for other in others_x:
            other_rows = pl.ds(pl.multiple_of(other * rows, rows), rows)
            remote(
                kv.at[j, :, other_rows], kv.at[j, :, other_rows],
                s_send.at[other, j], s_recv.at[other, j], space=other,
            ).wait_recv()
        query = squery[j]
        scores = lax.dot_general(
            query, kv[j, 0], (((1,), (1,)), ((), ())), preferred_element_type=jnp.float32
        ) * scale
        peak = jnp.max(scores, axis=1, keepdims=True)
        weights = jnp.exp(scores - peak)
        total = jnp.sum(weights, axis=1, keepdims=True)
        acc = jnp.dot(weights.astype(jnp.bfloat16), kv[j, 1], preferred_element_type=jnp.float32)
        res[c * here + j] = (acc / total).astype(jnp.bfloat16)

        for other in far_first:
            out_copy(j, other).start()

        @pl.when(j > 0)
        def _():
            for other in others_c:
                back_copy(j - 1, other).start()

        return 0

    lax.fori_loop(0, share, step, 0)
    for other in others_c:
        back_copy(share - 1, other).start()

    def forward(j, _):
        for other in others_f:
            theirs = pl.ds(pl.multiple_of(other * part, part), part)
            remote(
                tout.at[j, other], res.at[c * here + share + j, theirs], o_send.at[other, j], o_recv.at[other, j],
                frame=other,
            ).wait_recv()
        for other in others_c:
            back_copy(share + j, other).start()
        return 0

    lax.fori_loop(0, share, forward, 0)

    def arrive(slot, _):
        for other in others_c:
            remote(
                res.at[c * here + slot], res.at[other * here + slot], r_send.at[other, slot], r_recv.at[other, slot], head=other
            ).wait_recv()
        return 0

    lax.fori_loop(0, 2 * share, arrive, 0)

    for i in range(here):
        out_ref[0, :, i * HD:(i + 1) * HD] = res[place[c * here + i]]


    def drain(j, _):
        core_copy(j).wait_send()
        for other in others_f:
            window_copy(j, other).wait_send()
            out_copy(j, other).wait_send()
        for other in others_x:
            space_copy(j, other).wait_send()
        for other in others_c:
            back_copy(j, other).wait_send()
            back_copy(share + j, other).wait_send()
        return 0

    lax.fori_loop(0, share, drain, 0)


def direct_kernel(
    frames, spaces, cores, fulls, nears, tab, q_ref, k_ref, v_ref, out_ref,
    full, kv, tsend, trecv, tout, res, nsend, nrecv,
    loc_sem, word, s_send, s_recv, t_send, t_recv, o_send, o_recv, n_send, n_recv,
):
    rows = q_ref.shape[1]
    here = q_ref.shape[2] // HD
    part = rows // frames
    scale = HD ** (-0.5)
    f = lax.axis_index("frame")
    x = lax.axis_index("space")
    c = lax.axis_index("head")
    side = f // (frames // 2)

    def each(lower, upper, body):
        def run(i, _):
            body(i)
            return 0

        lax.fori_loop(lower, upper, run, 0)

    def of_core(counts):
        total = jnp.int32(counts[0])
        for e in range(1, cores):
            total = jnp.where(c == e, jnp.int32(counts[e]), total)
        return total

    n_full = of_core(fulls)
    n_near = of_core(nears)
    n_time = n_full + n_near
    n_space = here - n_time

    def remote(src, dst, send, recv, **target):
        return pltpu.make_async_remote_copy(
            src_ref=src, dst_ref=dst, send_sem=send, recv_sem=recv,
            device_id=target, device_id_type=MESH,
        )

    def lanes(h):
        return pl.ds(pl.multiple_of(h * HD, HD), HD)

    def there(way, d):
        other = f + (2 * way - 1) * d
        return (other >= 0) & (other < frames)

    def away(way, d):
        return jnp.clip(f + (2 * way - 1) * d, 0, frames - 1)

    barrier = pltpu.get_barrier_semaphore()
    for d in range(1, spaces):
        pl.semaphore_signal(
            barrier, inc=1, device_id={"space": lax.rem(x + d, spaces)}, device_id_type=MESH
        )
    for way in range(2):
        @pl.when(there(way, 1))
        def _():
            pl.semaphore_signal(barrier, inc=1, device_id={"frame": away(way, 1)}, device_id_type=MESH)

    def all_in(view, sem):
        pltpu.make_async_copy(view, view, sem).wait()

    for n, src in enumerate((k_ref, v_ref, q_ref)):
        each(0, here, lambda h: pltpu.make_async_copy(
            src.at[0, :, lanes(h)], full.at[n, h], loc_sem.at[0]).start())
    all_in(full, loc_sem.at[0])

    pl.semaphore_wait(
        barrier, spaces - 1 + there(0, 1).astype(jnp.int32) + there(1, 1).astype(jnp.int32)
    )

    def tell(way, d):
        @pl.when(there(way, d) & there(1 - way, 1))
        def _():
            pl.semaphore_signal(
                word.at[way, d - 1], inc=1, device_id={"frame": away(1 - way, 1)}, device_id_type=MESH
            )

    if frames > 2:
        for way in range(2):
            tell(way, 1)

    my_rows = pl.ds(pl.multiple_of(x * rows, rows), rows)
    mine = pl.ds(pl.multiple_of(f * part, part), part)

    def window_copy(j, other):
        return remote(
            tsend.at[j, other], trecv.at[f, j], t_send.at[0], t_recv.at[j], frame=other
        )

    def space_copy(j, other):
        return remote(
            kv.at[j, :, my_rows], kv.at[j, :, my_rows], s_send.at[0], s_recv.at[j], space=other
        )

    def out_copy(j, other):
        return remote(
            tout.at[j, other], res.at[j, mine], o_send.at[0], o_recv.at[0], frame=other
        )

    def near_copy(j, way):
        return remote(
            nsend.at[j], nrecv.at[1 - way, j], n_send.at[way], n_recv.at[1 - way], frame=away(way, 1)
        )

    def other_spaces(body):
        each(1, spaces, lambda d: body(lax.rem(x + d, spaces)))

    def far_first(body):
        each(0, frames - 1, lambda i: body(
            lax.rem(f + (1 - side) * (frames - 1 - i) + side * (1 + i), frames)))

    def head_of(slot):
        return tab[slot]

    def send_at(j, d):
        def one(way):
            @pl.when(there(way, d))
            def _():
                window_copy(j, away(way, d)).start()

        each(0, 2, one)

    def prepare_space(j):
        head = head_of(n_time + j)
        for n in range(2):
            kv[j, n, my_rows] = full[n, head]
        other_spaces(lambda other: space_copy(j, other).start())

    def prepare(j):
        @pl.when(j < n_full)
        def _():
            head = head_of(j)
            for n in range(3):
                block = full[n, head]
                for g in range(frames):
                    tsend[j, g, n] = block[g * part:(g + 1) * part]
            send_at(j, 1)

        @pl.when(j == EARLY - 1)
        def _():
            each(0, n_space, prepare_space)
            for d in range(2, frames):
                for way in range(2):
                    @pl.when(there(way, d))
                    def _():
                        pl.semaphore_wait(word.at[way, d - 2], 1)

                    if d < frames - 1:
                        tell(way, d)

        @pl.when(j >= EARLY - 1)
        def _():
            each(2, frames, lambda i: send_at(j - EARLY + 1, frames + 1 - i))

    each(0, n_full + EARLY - 1, prepare)

    def prepare_near(j):
        head = head_of(n_full + j)
        for n in range(2):
            nsend[j, n] = full[n, head]

        def one(way):
            @pl.when(there(way, 1))
            def _():
                near_copy(j, way).start()

        each(0, 2, one)

    if max(nears) > 0:
        each(0, n_near, prepare_near)

    fine = min(part, 16)
    wide = min(rows, 128)

    def weigh(scores, values):
        peak = functools.reduce(jnp.maximum, scores)
        weights = [jnp.exp(s - peak) for s in scores]
        total = functools.reduce(jnp.add, weights)
        acc = functools.reduce(
            jnp.add,
            [w.astype(jnp.bfloat16).astype(jnp.float32) * v for w, v in zip(weights, values)],
        )
        return (acc / total).astype(jnp.bfloat16)

    def step(j):
        @pl.when(j < n_full)
        def _():
            all_in(trecv.at[pl.ds(0, frames - 1), j], t_recv.at[j])
            trecv[f, j] = tsend[j, f]
            reach = tab[2 * here + j]

            def rows_step(i):
                at = pl.ds(pl.multiple_of(i * fine, fine), fine)
                qs = [trecv[g, j, 2, at].astype(jnp.float32) for g in range(frames)]
                ks = [trecv[g, j, 0, at].astype(jnp.float32) for g in range(frames)]
                vs = [trecv[g, j, 1, at].astype(jnp.float32) for g in range(frames)]
                for g in range(frames):
                    close = [m for m in range(frames) if abs(m - g) <= WMAX]
                    scores = []
                    for m in close:
                        raw = jnp.sum(qs[g] * ks[m], axis=-1, keepdims=True) * scale
                        scores.append(jnp.where(reach >= abs(m - g), raw, -1e30))
                    tout[j, g, at] = weigh(scores, [vs[m] for m in close])

            each(0, part // fine, rows_step)
            res[j, mine] = tout[j, f]
            far_first(lambda other: out_copy(j, other).start())

        @pl.when(j < n_space)
        def _():
            all_in(kv.at[j, :, pl.ds(0, (spaces - 1) * rows)], s_recv.at[j])
            head = head_of(n_time + j)

            def query_step(i):
                at = pl.ds(pl.multiple_of(i * wide, wide), wide)
                scores = lax.dot_general(
                    full[2, head, at], kv[j, 0], (((1,), (1,)), ((), ())), preferred_element_type=jnp.float32
                ) * scale
                peak = jnp.max(scores, axis=1, keepdims=True)
                weights = jnp.exp(scores - peak)
                total = jnp.sum(weights, axis=1, keepdims=True)
                acc = jnp.dot(weights.astype(jnp.bfloat16), kv[j, 1], preferred_element_type=jnp.float32)
                res[n_time + j, at] = (acc / total).astype(jnp.bfloat16)

            each(0, rows // wide, query_step)

    each(0, here, step)

    def by_core(counts, body):
        for e in range(cores):
            if counts[e] > 0:
                @pl.when(c == e)
                def _():
                    body(counts[e])

    def near_arrivals(count):
        for way in range(2):
            @pl.when(there(way, 1))
            def _():
                all_in(nrecv.at[way, pl.ds(0, count)], n_recv.at[way])

            @pl.when(jnp.logical_not(there(way, 1)))
            def _():
                nrecv[way, pl.ds(0, count)] = nsend[pl.ds(0, count)]

    by_core(nears, near_arrivals)

    def near_step(j):
        head = head_of(n_full + j)

        def rows_step(i):
            at = pl.ds(pl.multiple_of(i * fine, fine), fine)
            query = full[2, head, at].astype(jnp.float32)
            keys = (nrecv[0, j, 0, at], nsend[j, 0, at], nrecv[1, j, 0, at])
            values = (nrecv[0, j, 1, at], nsend[j, 1, at], nrecv[1, j, 1, at])
            scores = []
            for key, take in zip(keys, (there(0, 1), None, there(1, 1))):
                raw = jnp.sum(query * key.astype(jnp.float32), axis=-1, keepdims=True) * scale
                scores.append(raw if take is None else jnp.where(take, raw, -1e30))
            res[n_full + j, at] = weigh(scores, [v.astype(jnp.float32) for v in values])

        each(0, rows // fine, rows_step)

    if max(nears) > 0:
        each(0, n_near, near_step)

    by_core(fulls, lambda count: all_in(res.at[pl.ds(0, count), pl.ds(0, rows - part)], o_recv.at[0]))

    def place(i):
        out_ref[0, :, lanes(i)] = res[tab[here + i]]

    each(0, here, place)

    def near_sent(count):
        for way in range(2):
            @pl.when(there(way, 1))
            def _():
                all_in(nsend.at[pl.ds(0, count)], n_send.at[way])

    by_core(fulls, lambda count: all_in(tsend.at[pl.ds(0, count), pl.ds(0, frames - 1)], t_send.at[0]))
    by_core(fulls, lambda count: all_in(tout.at[pl.ds(0, count), pl.ds(0, frames - 1)], o_send.at[0]))
    by_core(
        [here - t - n for t, n in zip(fulls, nears)],
        lambda count: [all_in(kv.at[pl.ds(0, count), :, pl.ds(0, rows)], s_send.at[0]) for _ in range(1, spaces)],
    )
    by_core(nears, near_sent)


def direct(sizes, times, nears, number, queries, key_states, value_states, profile, window, table):
    frames, spaces, cores = sizes
    rows = queries.shape[1]
    here = queries.shape[2] // HD
    part = rows // frames
    fulls = tuple(t - n for t, n in zip(times, nears))
    most_full, most_near = max(1, *fulls), max(1, *nears)
    most_space = max(1, *(here - t for t in times))
    bf = jnp.bfloat16
    dma = pltpu.SemaphoreType.DMA
    return pl.pallas_call(
        functools.partial(direct_kernel, frames, spaces, cores, fulls, nears),
        out_shape=pltpu.VMEM(queries.shape, queries.dtype),
        in_specs=[pl.BlockSpec(memory_space=pltpu.SMEM)] + [pl.BlockSpec(memory_space=pltpu.HBM)] * 3,
        out_specs=pl.BlockSpec(memory_space=pltpu.VMEM),
        scratch_shapes=[
            pltpu.VMEM((3, here, rows, HD), bf),
            pltpu.VMEM((most_space, 2, spaces * rows, HD), bf),
            pltpu.VMEM((most_full, frames, 3, part, HD), bf),
            pltpu.VMEM((frames, most_full, 3, part, HD), bf),
            pltpu.VMEM((most_full, frames, part, HD), bf),
            pltpu.VMEM((here, rows, HD), bf),
            pltpu.VMEM((most_near, 2, rows, HD), bf),
            pltpu.VMEM((2, most_near, 2, rows, HD), bf),
            dma((1,)),
            pltpu.SemaphoreType.REGULAR((2, max(1, frames - 2))),
            dma((1,)),
            dma((most_space,)),
            dma((1,)),
            dma((most_full,)),
            dma((1,)),
            dma((1,)),
            dma((2,)),
            dma((2,)),
        ],
        compiler_params=pltpu.CompilerParams(
            collective_id=number, has_side_effects=True, vmem_limit_bytes=60 * 1024 * 1024
        ),
    )(table, queries, key_states, value_states)


def shared(sizes, queries, key_states, value_states, profile, window, table):
    frames, spaces, cores = sizes
    rows = queries.shape[1]
    here = queries.shape[2] // HD
    share = here // 2
    part = rows // frames
    any_space = pl.BlockSpec(memory_space=pltpu.HBM)
    bf = jnp.bfloat16
    dma = pltpu.SemaphoreType.DMA
    return pl.pallas_call(
        functools.partial(shared_kernel, frames, spaces, cores),
        out_shape=pltpu.VMEM(queries.shape, queries.dtype),
        in_specs=[pl.BlockSpec(memory_space=pltpu.VMEM)] * 2 + [any_space] * 3,
        out_specs=pl.BlockSpec(memory_space=pltpu.VMEM),
        scratch_shapes=[
            pltpu.VMEM((3, here, rows, HD), bf),
            pltpu.VMEM((here, 3, rows, HD), bf),
            pltpu.VMEM((share, 3, rows, HD), bf),
            pltpu.VMEM((share, rows, HD), bf),
            pltpu.VMEM((share, 2, spaces * rows, HD), bf),
            pltpu.VMEM((share, frames, 3, part, HD), bf),
            pltpu.VMEM((frames, share, 3, part, HD), bf),
            pltpu.VMEM((share, frames, part, HD), bf),
            pltpu.VMEM((cores * 2 * share, rows, HD), bf),
            pltpu.SMEM((here * cores,), jnp.int32),
            pltpu.SMEM((here * cores,), jnp.int32),
            pltpu.SMEM((here * cores,), jnp.int32),
            pltpu.SMEM((here * cores,), jnp.int32),
            pltpu.SMEM((here,), jnp.int32),
            pltpu.SMEM((share,), jnp.int32),
            dma((5,)),
            dma((share,)),
            dma((share,)),
            dma((spaces, share)),
            dma((spaces, share)),
            dma((frames, share)),
            dma((frames, share)),
            dma((frames, share)),
            dma((frames, share)),
            dma((cores, 2 * share)),
            dma((cores, 2 * share)),
        ],
        compiler_params=pltpu.CompilerParams(
            collective_id=0, has_side_effects=True, vmem_limit_bytes=60 * 1024 * 1024
        ),
    )(profile, window, queries, key_states, value_states)


def choose_kernel(
    cores, caps, prof_ref, win_ref, prof_hbm, win_hbm, out_ref, tab, prof_out, win_out, sem
):
    here = prof_ref.shape[0] // cores
    c = lax.axis_index("head")
    copies = (
        pltpu.make_async_copy(prof_hbm, prof_out, sem.at[0]),
        pltpu.make_async_copy(win_hbm, win_out, sem.at[1]),
    )
    for copy in copies:
        copy.start()
    first = jnp.int32(0)
    for h in range(here):
        first = first + 1 - prof_ref[h]
    nears = []
    for e in range(cores):
        near = jnp.int32(0)
        for h in range(e * here, (e + 1) * here):
            near = near + (1 - prof_ref[h]) * (win_ref[h] == 1).astype(jnp.int32)
        nears.append(near)
    index = jnp.int32(0)
    base = 1
    for count, cap in caps.items():
        here_index = jnp.int32(0)
        for near in nears:
            here_index = here_index * (cap + 1) + jnp.minimum(near, cap)
        index = jnp.where(first == count, base + here_index, index)
        base = base + (cap + 1) ** cores
    out_ref[0] = index

    kinds = []
    for h in range(here):
        p = prof_ref[c * here + h]
        kinds.append(p * 2 + (1 - p) * (win_ref[c * here + h] == 1).astype(jnp.int32))
    tops = [jnp.int32(0)]
    for kind in range(2):
        top = tops[-1]
        for h in range(here):
            top = top + (kinds[h] == kind).astype(jnp.int32)
        tops.append(top)
    for h in range(here):
        slot = jnp.where(kinds[h] == 0, tops[0], jnp.where(kinds[h] == 1, tops[1], tops[2]))
        for kind in range(3):
            tops[kind] = tops[kind] + (kinds[h] == kind).astype(jnp.int32)
        tab[slot] = h
        tab[here + h] = slot
        tab[2 * here + slot] = win_ref[c * here + h]
    for copy in copies:
        copy.wait()


def local(sizes, queries, key_states, value_states, profile, window):
    frames, spaces, cores = sizes
    here = queries.shape[2] // HD
    caps = {here // 2 + d: cap for d, cap in CAPS.items()}
    smem = pl.BlockSpec(memory_space=pltpu.SMEM)
    vmem = pl.BlockSpec(memory_space=pltpu.VMEM)
    hbm = pl.BlockSpec(memory_space=pltpu.HBM)
    index, table, profile, window = pl.pallas_call(
        functools.partial(choose_kernel, cores, caps),
        out_shape=(
            pltpu.SMEM((1,), jnp.int32),
            pltpu.SMEM((3 * here,), jnp.int32),
            pltpu.VMEM(profile.shape, profile.dtype),
            pltpu.VMEM(window.shape, window.dtype),
        ),
        in_specs=[smem, smem, hbm, hbm],
        out_specs=(smem, smem, vmem, vmem),
        scratch_shapes=[pltpu.SemaphoreType.DMA((2,))],
    )(profile, window, profile, window)
    ways = [functools.partial(shared, sizes)]
    for first, cap in caps.items():
        for nears in itertools.product(range(cap + 1), repeat=cores):
            ways.append(functools.partial(direct, sizes, (first, here - first), nears, len(ways)))
    return lax.switch(index[0], ways, queries, key_states, value_states, profile, window, table)


def solution(mesh):
    spec = P(("groups", "frame"), "space", "head")
    sizes = (mesh.shape["frame"], mesh.shape["space"], mesh.shape["head"])
    return jax.shard_map(
        functools.partial(local, sizes),
        mesh=mesh,
        in_specs=(spec, spec, spec, P(), P()),
        out_specs=spec,
        check_vma=False,
    )
```

```python
import functools
import itertools

import jax
import jax.numpy as jnp
from jax import lax
from jax.experimental import pallas as pl
from jax.experimental.pallas import tpu as pltpu
from jax.sharding import PartitionSpec as P

HD = 128
WMAX = 4
CAPS = {0: (2, 2), -1: (2, 2), 1: (2, 2), -2: (1, 2), 2: (0, 1)}
EARLY = 2
MESH = pl.DeviceIdType.MESH


def shared_kernel(
    frames, spaces, cores, prof_hbm, win_hbm, q_ref, k_ref, v_ref, out_ref,
    full, mine_first, theirs, squery, kv, tsend, trecv, tout, res,
    prof_ref, win_ref, pos, place, order, tab,
    loc_sem, d_send, d_recv, s_send, s_recv, t_send, t_recv, o_send, o_recv, r_send, r_recv,
):
    rows = q_ref.shape[1]
    here = q_ref.shape[2] // HD
    share = here // 2
    part = rows // frames
    scale = HD ** (-0.5)
    f = lax.axis_index("frame")
    x = lax.axis_index("space")
    c = lax.axis_index("head")
    others_f = [lax.rem(f + d, frames) for d in range(1, frames)]
    others_x = [lax.rem(x + d, spaces) for d in range(1, spaces)]
    others_c = [lax.rem(c + d, cores) for d in range(1, cores)]
    side = f // (frames // 2)
    far_first = [
        lax.rem(f + (1 - side) * (frames - 1 - i) + side * (1 + i), frames)
        for i in range(frames - 1)
    ]

    def remote(src, dst, send, recv, **target):
        return pltpu.make_async_remote_copy(
            src_ref=src, dst_ref=dst, send_sem=send, recv_sem=recv,
            device_id=target, device_id_type=MESH,
        )

    def lanes(h):
        return pl.ds(pl.multiple_of(h * HD, HD), HD)

    small = (
        pltpu.make_async_copy(prof_hbm, prof_ref, loc_sem.at[3]),
        pltpu.make_async_copy(win_hbm, win_ref, loc_sem.at[4]),
    )
    for copy in small:
        copy.start()
    sources = (k_ref, v_ref, q_ref)
    for n, src in enumerate(sources):
        def local_start(h, _):
            pltpu.make_async_copy(src.at[0, :, lanes(h)], full.at[n, h], loc_sem.at[n]).start()
            return 0

        lax.fori_loop(0, here, local_start, 0)

    barrier = pltpu.get_barrier_semaphore()
    for other in others_c:
        pl.semaphore_signal(barrier, inc=1, device_id={"head": other}, device_id_type=MESH)
    for other in others_x:
        pl.semaphore_signal(barrier, inc=1, device_id={"space": other}, device_id_type=MESH)
    for other in others_f:
        pl.semaphore_signal(barrier, inc=1, device_id={"frame": other}, device_id_type=MESH)

    for copy in small:
        copy.wait()

    count = jnp.int32(0)
    for h in range(here):
        count = count + prof_ref[h]
    first_space = (count >= share).astype(jnp.int32)
    main_count = jnp.maximum(count, here - count)
    for e in range(cores):
        main = first_space if e == 0 else 1 - first_space
        major = jnp.int32(0)
        minor = main_count
        for h in range(here):
            p = prof_ref[e * here + h]
            is_main = p * main + (1 - p) * (1 - main)
            slot = jnp.clip(is_main * major + (1 - is_main) * minor, 0, here - 1)
            major = major + is_main
            minor = minor + (1 - is_main)
            away = ((slot >= share) & (slot < main_count)).astype(jnp.int32)
            owner = away * (1 - e) + (1 - away) * e
            pos[e * here + h] = slot
            place[e * here + h] = owner * here + (1 - p) * share + slot - (slot >= share).astype(jnp.int32) * share

    def fill(slot, _):
        head = jnp.int32(0)
        for h in range(here):
            head = head + jnp.where(pos[c * here + h] == slot, h, 0)
        order[slot] = jnp.clip(head, 0, here - 1)
        return 0

    lax.fori_loop(0, here, fill, 0)

    for n in range(3):
        pltpu.make_async_copy(full.at[n], full.at[n], loc_sem.at[n]).wait()

    def arrange(slot, _):
        head = order[slot]
        for n in range(3):
            mine_first[slot, n] = full[n, head]
        return 0

    lax.fori_loop(0, here, arrange, 0)

    pl.semaphore_wait(barrier, len(others_c) + len(others_x) + len(others_f))

    partner = others_c[0]

    def core_copy(j):
        return remote(mine_first.at[share + j], theirs.at[j], d_send.at[j], d_recv.at[j], head=partner)

    def core_start(j, _):
        core_copy(j).start()
        return 0

    lax.fori_loop(0, share, core_start, 0)

    main_space = c * (1 - first_space) + (1 - c) * first_space
    my_rows = pl.ds(pl.multiple_of(x * rows, rows), rows)
    mine = pl.ds(pl.multiple_of(f * part, part), part)

    def window_copy(j, other):
        return remote(
            tsend.at[j, other], trecv.at[f, j], t_send.at[other, j], t_recv.at[f, j], frame=other
        )

    def space_copy(j, other):
        return remote(
            kv.at[j, :, my_rows], kv.at[j, :, my_rows], s_send.at[other, j], s_recv.at[x, j], space=other
        )

    def gather(j, _):
        core_copy(j).wait_recv()
        borrowed = share + j < main_count
        for n in range(3):
            head_main = mine_first[j, n]
            head_rest = jnp.where(borrowed, theirs[j, n], mine_first[share + j, n])
            block = jnp.where(main_space == 1, head_rest, head_main)
            for g in range(frames):
                tsend[j, g, n] = block[g * part:(g + 1) * part]
            block = jnp.where(main_space == 1, head_main, head_rest)
            if n < 2:
                kv[j, n, my_rows] = block
            else:
                squery[j] = block
        for other in far_first:
            window_copy(j, other).start()

        @pl.when(j > 0)
        def _():
            for other in others_x:
                space_copy(j - 1, other).start()

        return 0

    lax.fori_loop(0, share, gather, 0)

    def fill_reach(j, _):
        own_slot = j + main_space * share
        far = ((main_space == 1) & (share + j < main_count)).astype(jnp.int32)
        own_reach = jnp.int32(0)
        far_reach = jnp.int32(0)
        for h in range(here):
            own_reach = own_reach + jnp.where(pos[c * here + h] == own_slot, win_ref[c * here + h], 0)
            far_reach = far_reach + jnp.where(
                pos[partner * here + h] == share + j, win_ref[partner * here + h], 0
            )
        tab[j] = far * far_reach + (1 - far) * own_reach
        return 0

    lax.fori_loop(0, share, fill_reach, 0)

    def out_copy(j, other):
        return remote(
            tout.at[j, other], res.at[c * here + share + j, mine], o_send.at[other, j], o_recv.at[f, j], frame=other
        )

    def back_copy(slot, other):
        return remote(
            res.at[c * here + slot], res.at[c * here + slot], r_send.at[other, slot], r_recv.at[c, slot], head=other
        )

    for other in others_x:
        space_copy(share - 1, other).start()

    def step(j, _):
        for other in others_f:
            remote(
                tsend.at[j, other], trecv.at[other, j], t_send.at[other, j], t_recv.at[other, j], frame=other
            ).wait_recv()
        trecv[f, j] = tsend[j, f]
        reach = tab[j]
        qs = [trecv[g, j, 2].astype(jnp.float32) for g in range(frames)]
        ks = [trecv[g, j, 0].astype(jnp.float32) for g in range(frames)]
        vs = [trecv[g, j, 1].astype(jnp.float32) for g in range(frames)]
        for g in range(frames):
            near = [m for m in range(frames) if abs(m - g) <= WMAX]
            scores = []
            for m in near:
                raw = jnp.sum(qs[g] * ks[m], axis=-1, keepdims=True) * scale
                scores.append(jnp.where(reach >= abs(m - g), raw, -1e30))
            peak = functools.reduce(jnp.maximum, scores)
            weights = [jnp.exp(s - peak) for s in scores]
            total = functools.reduce(jnp.add, weights)
            acc = functools.reduce(
                jnp.add,
                [w.astype(jnp.bfloat16).astype(jnp.float32) * vs[m] for w, m in zip(weights, near)],
            )
            tout[j, g] = (acc / total).astype(jnp.bfloat16)
        res[c * here + share + j, mine] = tout[j, f]

        for other in others_x:
            other_rows = pl.ds(pl.multiple_of(other * rows, rows), rows)
            remote(
                kv.at[j, :, other_rows], kv.at[j, :, other_rows],
                s_send.at[other, j], s_recv.at[other, j], space=other,
            ).wait_recv()
        query = squery[j]
        scores = lax.dot_general(
            query, kv[j, 0], (((1,), (1,)), ((), ())), preferred_element_type=jnp.float32
        ) * scale
        peak = jnp.max(scores, axis=1, keepdims=True)
        weights = jnp.exp(scores - peak)
        total = jnp.sum(weights, axis=1, keepdims=True)
        acc = jnp.dot(weights.astype(jnp.bfloat16), kv[j, 1], preferred_element_type=jnp.float32)
        res[c * here + j] = (acc / total).astype(jnp.bfloat16)

        for other in far_first:
            out_copy(j, other).start()

        @pl.when(j > 0)
        def _():
            for other in others_c:
                back_copy(j - 1, other).start()

        return 0

    lax.fori_loop(0, share, step, 0)
    for other in others_c:
        back_copy(share - 1, other).start()

    def forward(j, _):
        for other in others_f:
            theirs = pl.ds(pl.multiple_of(other * part, part), part)
            remote(
                tout.at[j, other], res.at[c * here + share + j, theirs], o_send.at[other, j], o_recv.at[other, j],
                frame=other,
            ).wait_recv()
        for other in others_c:
            back_copy(share + j, other).start()
        return 0

    lax.fori_loop(0, share, forward, 0)

    def arrive(slot, _):
        for other in others_c:
            remote(
                res.at[c * here + slot], res.at[other * here + slot], r_send.at[other, slot], r_recv.at[other, slot], head=other
            ).wait_recv()
        return 0

    lax.fori_loop(0, 2 * share, arrive, 0)

    for i in range(here):
        out_ref[i] = res[place[c * here + i]]


    def drain(j, _):
        core_copy(j).wait_send()
        for other in others_f:
            window_copy(j, other).wait_send()
            out_copy(j, other).wait_send()
        for other in others_x:
            space_copy(j, other).wait_send()
        for other in others_c:
            back_copy(j, other).wait_send()
            back_copy(share + j, other).wait_send()
        return 0

    lax.fori_loop(0, share, drain, 0)


def direct_kernel(
    frames, spaces, cores, fulls, nears, tab, q_ref, k_ref, v_ref, res,
    full, kv, tsend, trecv, tout, nsend, nrecv,
    loc_sem, word, s_send, s_recv, t_send, t_recv, o_send, o_recv, n_send, n_recv,
):
    rows = q_ref.shape[1]
    here = q_ref.shape[2] // HD
    part = rows // frames
    scale = HD ** (-0.5)
    f = lax.axis_index("frame")
    x = lax.axis_index("space")
    c = lax.axis_index("head")
    side = f // (frames // 2)

    def each(lower, upper, body):
        def run(i, _):
            body(i)
            return 0

        lax.fori_loop(lower, upper, run, 0)

    def of_core(counts):
        total = jnp.int32(counts[0])
        for e in range(1, cores):
            total = jnp.where(c == e, jnp.int32(counts[e]), total)
        return total

    n_full = of_core(fulls)
    n_near = of_core(nears)
    n_time = n_full + n_near
    n_space = here - n_time

    def remote(src, dst, send, recv, **target):
        return pltpu.make_async_remote_copy(
            src_ref=src, dst_ref=dst, send_sem=send, recv_sem=recv,
            device_id=target, device_id_type=MESH,
        )

    def lanes(h):
        return pl.ds(pl.multiple_of(h * HD, HD), HD)

    def there(way, d):
        other = f + (2 * way - 1) * d
        return (other >= 0) & (other < frames)

    def away(way, d):
        return jnp.clip(f + (2 * way - 1) * d, 0, frames - 1)

    barrier = pltpu.get_barrier_semaphore()
    for d in range(1, spaces):
        pl.semaphore_signal(
            barrier, inc=1, device_id={"space": lax.rem(x + d, spaces)}, device_id_type=MESH
        )
    for way in range(2):
        @pl.when(there(way, 1))
        def _():
            pl.semaphore_signal(barrier, inc=1, device_id={"frame": away(way, 1)}, device_id_type=MESH)

    def all_in(view, sem):
        pltpu.make_async_copy(view, view, sem).wait()

    for n, src in enumerate((k_ref, v_ref, q_ref)):
        each(0, here, lambda h: pltpu.make_async_copy(
            src.at[0, :, lanes(h)], full.at[n, h], loc_sem.at[0]).start())
    all_in(full, loc_sem.at[0])

    pl.semaphore_wait(
        barrier, spaces - 1 + there(0, 1).astype(jnp.int32) + there(1, 1).astype(jnp.int32)
    )

    def tell(way, d):
        @pl.when(there(way, d) & there(1 - way, 1))
        def _():
            pl.semaphore_signal(
                word.at[way, d - 1], inc=1, device_id={"frame": away(1 - way, 1)}, device_id_type=MESH
            )

    if frames > 2:
        for way in range(2):
            tell(way, 1)

    my_rows = pl.ds(pl.multiple_of(x * rows, rows), rows)
    mine = pl.ds(pl.multiple_of(f * part, part), part)

    def window_copy(j, other):
        return remote(
            tsend.at[j, other], trecv.at[f, j], t_send.at[0], t_recv.at[j], frame=other
        )

    def space_copy(j, other):
        return remote(
            kv.at[j, :, my_rows], kv.at[j, :, my_rows], s_send.at[0], s_recv.at[j], space=other
        )

    def out_copy(j, other):
        return remote(
            tout.at[j, other], res.at[j, mine], o_send.at[0], o_recv.at[0], frame=other
        )

    def near_copy(j, way):
        return remote(
            nsend.at[j], nrecv.at[1 - way, j], n_send.at[way], n_recv.at[1 - way], frame=away(way, 1)
        )

    def other_spaces(body):
        each(1, spaces, lambda d: body(lax.rem(x + d, spaces)))

    def far_first(body):
        each(0, frames - 1, lambda i: body(
            lax.rem(f + (1 - side) * (frames - 1 - i) + side * (1 + i), frames)))

    def head_of(slot):
        return tab[slot]

    def send_at(j, d):
        def one(way):
            @pl.when(there(way, d))
            def _():
                window_copy(j, away(way, d)).start()

        each(0, 2, one)

    def prepare_space(j):
        head = head_of(n_time + j)
        for n in range(2):
            kv[j, n, my_rows] = full[n, head]
        other_spaces(lambda other: space_copy(j, other).start())

    def prepare(j):
        @pl.when(j < n_full)
        def _():
            head = head_of(j)
            for n in range(3):
                block = full[n, head]
                for g in range(frames):
                    tsend[j, g, n] = block[g * part:(g + 1) * part]
            send_at(j, 1)

        @pl.when(j == EARLY - 1)
        def _():
            each(0, n_space, prepare_space)
            for d in range(2, frames):
                for way in range(2):
                    @pl.when(there(way, d))
                    def _():
                        pl.semaphore_wait(word.at[way, d - 2], 1)

                    if d < frames - 1:
                        tell(way, d)

        @pl.when(j >= EARLY - 1)
        def _():
            each(2, frames, lambda i: send_at(j - EARLY + 1, frames + 1 - i))

    each(0, n_full + EARLY - 1, prepare)

    def prepare_near(j):
        head = head_of(n_full + j)
        for n in range(2):
            nsend[j, n] = full[n, head]

        def one(way):
            @pl.when(there(way, 1))
            def _():
                near_copy(j, way).start()

        each(0, 2, one)

    if max(nears) > 0:
        each(0, n_near, prepare_near)

    fine = min(part, 16)
    wide = min(rows, 128)

    def weigh(scores, values):
        peak = functools.reduce(jnp.maximum, scores)
        weights = [jnp.exp(s - peak) for s in scores]
        total = functools.reduce(jnp.add, weights)
        acc = functools.reduce(
            jnp.add,
            [w.astype(jnp.bfloat16).astype(jnp.float32) * v for w, v in zip(weights, values)],
        )
        return (acc / total).astype(jnp.bfloat16)

    def step(j):
        @pl.when(j < n_full)
        def _():
            all_in(trecv.at[pl.ds(0, frames - 1), j], t_recv.at[j])
            trecv[f, j] = tsend[j, f]
            reach = tab[2 * here + j]

            def rows_step(i):
                at = pl.ds(pl.multiple_of(i * fine, fine), fine)
                qs = [trecv[g, j, 2, at].astype(jnp.float32) for g in range(frames)]
                ks = [trecv[g, j, 0, at].astype(jnp.float32) for g in range(frames)]
                vs = [trecv[g, j, 1, at].astype(jnp.float32) for g in range(frames)]
                for g in range(frames):
                    close = [m for m in range(frames) if abs(m - g) <= WMAX]
                    scores = []
                    for m in close:
                        raw = jnp.sum(qs[g] * ks[m], axis=-1, keepdims=True) * scale
                        scores.append(jnp.where(reach >= abs(m - g), raw, -1e30))
                    tout[j, g, at] = weigh(scores, [vs[m] for m in close])

            each(0, part // fine, rows_step)
            res[j, mine] = tout[j, f]
            far_first(lambda other: out_copy(j, other).start())

        @pl.when(j < n_space)
        def _():
            all_in(kv.at[j, :, pl.ds(0, (spaces - 1) * rows)], s_recv.at[j])
            head = head_of(n_time + j)

            def query_step(i):
                at = pl.ds(pl.multiple_of(i * wide, wide), wide)
                scores = lax.dot_general(
                    full[2, head, at], kv[j, 0], (((1,), (1,)), ((), ())), preferred_element_type=jnp.float32
                ) * scale
                peak = jnp.max(scores, axis=1, keepdims=True)
                weights = jnp.exp(scores - peak)
                total = jnp.sum(weights, axis=1, keepdims=True)
                acc = jnp.dot(weights.astype(jnp.bfloat16), kv[j, 1], preferred_element_type=jnp.float32)
                res[n_time + j, at] = (acc / total).astype(jnp.bfloat16)

            each(0, rows // wide, query_step)

    each(0, here, step)

    def by_core(counts, body):
        for e in range(cores):
            if counts[e] > 0:
                @pl.when(c == e)
                def _():
                    body(counts[e])

    def near_arrivals(count):
        for way in range(2):
            @pl.when(there(way, 1))
            def _():
                all_in(nrecv.at[way, pl.ds(0, count)], n_recv.at[way])

            @pl.when(jnp.logical_not(there(way, 1)))
            def _():
                nrecv[way, pl.ds(0, count)] = nsend[pl.ds(0, count)]

    by_core(nears, near_arrivals)

    def near_step(j):
        head = head_of(n_full + j)

        def rows_step(i):
            at = pl.ds(pl.multiple_of(i * fine, fine), fine)
            query = full[2, head, at].astype(jnp.float32)
            keys = (nrecv[0, j, 0, at], nsend[j, 0, at], nrecv[1, j, 0, at])
            values = (nrecv[0, j, 1, at], nsend[j, 1, at], nrecv[1, j, 1, at])
            scores = []
            for key, take in zip(keys, (there(0, 1), None, there(1, 1))):
                raw = jnp.sum(query * key.astype(jnp.float32), axis=-1, keepdims=True) * scale
                scores.append(raw if take is None else jnp.where(take, raw, -1e30))
            res[n_full + j, at] = weigh(scores, [v.astype(jnp.float32) for v in values])

        each(0, rows // fine, rows_step)

    if max(nears) > 0:
        each(0, n_near, near_step)

    by_core(fulls, lambda count: all_in(res.at[pl.ds(0, count), pl.ds(0, rows - part)], o_recv.at[0]))


    def near_sent(count):
        for way in range(2):
            @pl.when(there(way, 1))
            def _():
                all_in(nsend.at[pl.ds(0, count)], n_send.at[way])

    by_core(fulls, lambda count: all_in(tsend.at[pl.ds(0, count), pl.ds(0, frames - 1)], t_send.at[0]))
    by_core(fulls, lambda count: all_in(tout.at[pl.ds(0, count), pl.ds(0, frames - 1)], o_send.at[0]))
    by_core(
        [here - t - n for t, n in zip(fulls, nears)],
        lambda count: [all_in(kv.at[pl.ds(0, count), :, pl.ds(0, rows)], s_send.at[0]) for _ in range(1, spaces)],
    )
    by_core(nears, near_sent)


def direct(sizes, times, nears, number, queries, key_states, value_states, profile, window, table):
    frames, spaces, cores = sizes
    rows = queries.shape[1]
    here = queries.shape[2] // HD
    part = rows // frames
    fulls = tuple(t - n for t, n in zip(times, nears))
    most_full, most_near = max(1, *fulls), max(1, *nears)
    most_space = max(1, *(here - t for t in times))
    bf = jnp.bfloat16
    dma = pltpu.SemaphoreType.DMA
    return pl.pallas_call(
        functools.partial(direct_kernel, frames, spaces, cores, fulls, nears),
        out_shape=pltpu.VMEM((here, rows, HD), queries.dtype),
        in_specs=[pl.BlockSpec(memory_space=pltpu.SMEM)] + [pl.BlockSpec(memory_space=pltpu.HBM)] * 3,
        out_specs=pl.BlockSpec(memory_space=pltpu.VMEM),
        scratch_shapes=[
            pltpu.VMEM((3, here, rows, HD), bf),
            pltpu.VMEM((most_space, 2, spaces * rows, HD), bf),
            pltpu.VMEM((most_full, frames, 3, part, HD), bf),
            pltpu.VMEM((frames, most_full, 3, part, HD), bf),
            pltpu.VMEM((most_full, frames, part, HD), bf),
            pltpu.VMEM((most_near, 2, rows, HD), bf),
            pltpu.VMEM((2, most_near, 2, rows, HD), bf),
            dma((1,)),
            pltpu.SemaphoreType.REGULAR((2, max(1, frames - 2))),
            dma((1,)),
            dma((most_space,)),
            dma((1,)),
            dma((most_full,)),
            dma((1,)),
            dma((1,)),
            dma((2,)),
            dma((2,)),
        ],
        compiler_params=pltpu.CompilerParams(
            collective_id=number, has_side_effects=True, vmem_limit_bytes=60 * 1024 * 1024
        ),
    )(table, queries, key_states, value_states)


def shared(sizes, queries, key_states, value_states, profile, window, table):
    frames, spaces, cores = sizes
    rows = queries.shape[1]
    here = queries.shape[2] // HD
    share = here // 2
    part = rows // frames
    any_space = pl.BlockSpec(memory_space=pltpu.HBM)
    bf = jnp.bfloat16
    dma = pltpu.SemaphoreType.DMA
    return pl.pallas_call(
        functools.partial(shared_kernel, frames, spaces, cores),
        out_shape=pltpu.VMEM((here, rows, HD), queries.dtype),
        in_specs=[pl.BlockSpec(memory_space=pltpu.VMEM)] * 2 + [any_space] * 3,
        out_specs=pl.BlockSpec(memory_space=pltpu.VMEM),
        scratch_shapes=[
            pltpu.VMEM((3, here, rows, HD), bf),
            pltpu.VMEM((here, 3, rows, HD), bf),
            pltpu.VMEM((share, 3, rows, HD), bf),
            pltpu.VMEM((share, rows, HD), bf),
            pltpu.VMEM((share, 2, spaces * rows, HD), bf),
            pltpu.VMEM((share, frames, 3, part, HD), bf),
            pltpu.VMEM((frames, share, 3, part, HD), bf),
            pltpu.VMEM((share, frames, part, HD), bf),
            pltpu.VMEM((cores * 2 * share, rows, HD), bf),
            pltpu.SMEM((here * cores,), jnp.int32),
            pltpu.SMEM((here * cores,), jnp.int32),
            pltpu.SMEM((here * cores,), jnp.int32),
            pltpu.SMEM((here * cores,), jnp.int32),
            pltpu.SMEM((here,), jnp.int32),
            pltpu.SMEM((share,), jnp.int32),
            dma((5,)),
            dma((share,)),
            dma((share,)),
            dma((spaces, share)),
            dma((spaces, share)),
            dma((frames, share)),
            dma((frames, share)),
            dma((frames, share)),
            dma((frames, share)),
            dma((cores, 2 * share)),
            dma((cores, 2 * share)),
        ],
        compiler_params=pltpu.CompilerParams(
            collective_id=0, has_side_effects=True, vmem_limit_bytes=60 * 1024 * 1024
        ),
    )(profile, window, queries, key_states, value_states)


def place_kernel(tab, res, out_ref, sem):
    here = res.shape[0]

    def put(slot, _):
        at = pl.ds(pl.multiple_of(tab[slot] * HD, HD), HD)
        pltpu.make_async_copy(res.at[slot], out_ref.at[0, :, at], sem.at[0]).start()
        return 0

    lax.fori_loop(0, here, put, 0)
    pltpu.make_async_copy(res, res, sem.at[0]).wait()


def choose_kernel(
    cores, caps, prof_ref, win_ref, prof_hbm, win_hbm, out_ref, tab, prof_out, win_out, sem
):
    here = prof_ref.shape[0] // cores
    c = lax.axis_index("head")
    copies = (
        pltpu.make_async_copy(prof_hbm, prof_out, sem.at[0]),
        pltpu.make_async_copy(win_hbm, win_out, sem.at[1]),
    )
    for copy in copies:
        copy.start()
    first = jnp.int32(0)
    for h in range(here):
        first = first + 1 - prof_ref[h]
    nears = []
    for e in range(cores):
        near = jnp.int32(0)
        for h in range(e * here, (e + 1) * here):
            near = near + (1 - prof_ref[h]) * (win_ref[h] == 1).astype(jnp.int32)
        nears.append(near)
    index = jnp.int32(0)
    base = 1
    for count, most in caps.items():
        here_index = jnp.int32(0)
        size = 1
        for near, cap in zip(nears, most):
            here_index = here_index * (cap + 1) + jnp.minimum(near, cap)
            size = size * (cap + 1)
        index = jnp.where(first == count, base + here_index, index)
        base = base + size
    out_ref[0] = index

    kinds = []
    for h in range(here):
        p = prof_ref[c * here + h]
        kinds.append(p * 2 + (1 - p) * (win_ref[c * here + h] == 1).astype(jnp.int32))
    tops = [jnp.int32(0)]
    for kind in range(2):
        top = tops[-1]
        for h in range(here):
            top = top + (kinds[h] == kind).astype(jnp.int32)
        tops.append(top)
    for h in range(here):
        slot = jnp.where(kinds[h] == 0, tops[0], jnp.where(kinds[h] == 1, tops[1], tops[2]))
        for kind in range(3):
            tops[kind] = tops[kind] + (kinds[h] == kind).astype(jnp.int32)
        tab[slot] = h
        tab[here + h] = slot
        tab[2 * here + slot] = win_ref[c * here + h]
    @pl.when(index == 0)
    def _():
        for h in range(here):
            tab[h] = h

    for copy in copies:
        copy.wait()


def local(sizes, queries, key_states, value_states, profile, window):
    frames, spaces, cores = sizes
    here = queries.shape[2] // HD
    caps = {here // 2 + d: most for d, most in CAPS.items()}
    smem = pl.BlockSpec(memory_space=pltpu.SMEM)
    vmem = pl.BlockSpec(memory_space=pltpu.VMEM)
    hbm = pl.BlockSpec(memory_space=pltpu.HBM)
    index, table, profile, window = pl.pallas_call(
        functools.partial(choose_kernel, cores, caps),
        out_shape=(
            pltpu.SMEM((1,), jnp.int32),
            pltpu.SMEM((3 * here,), jnp.int32),
            pltpu.VMEM(profile.shape, profile.dtype),
            pltpu.VMEM(window.shape, window.dtype),
        ),
        in_specs=[smem, smem, hbm, hbm],
        out_specs=(smem, smem, vmem, vmem),
        scratch_shapes=[pltpu.SemaphoreType.DMA((2,))],
    )(profile, window, profile, window)
    ways = [functools.partial(shared, sizes)]
    for first, most in caps.items():
        for nears in itertools.product(*(range(cap + 1) for cap in most)):
            ways.append(functools.partial(direct, sizes, (first, here - first), nears, len(ways)))
    result = lax.switch(index[0], ways, queries, key_states, value_states, profile, window, table)
    return pl.pallas_call(
        place_kernel,
        out_shape=jax.ShapeDtypeStruct(queries.shape, queries.dtype),
        in_specs=[smem, vmem],
        out_specs=hbm,
        scratch_shapes=[pltpu.SemaphoreType.DMA((1,))],
    )(table, result)


def solution(mesh):
    spec = P(("groups", "frame"), "space", "head")
    sizes = (mesh.shape["frame"], mesh.shape["space"], mesh.shape["head"])
    return jax.shard_map(
        functools.partial(local, sizes),
        mesh=mesh,
        in_specs=(spec, spec, spec, P(), P()),
        out_specs=spec,
        check_vma=False,
    )
```

```python
import functools
import itertools

import jax
import jax.numpy as jnp
from jax import lax
from jax.experimental import pallas as pl
from jax.experimental.pallas import tpu as pltpu
from jax.sharding import PartitionSpec as P

HD = 128
WMAX = 4
CAPS = {0: (2, 2), -1: (2, 2), 1: (2, 2), -2: (1, 2), 2: (0, 1)}
EARLY = 2
MESH = pl.DeviceIdType.MESH


def shared_kernel(
    frames, spaces, cores, prof_ref, win_ref, q_ref, k_ref, v_ref, out_ref,
    full, mine_first, theirs, squery, kv, tsend, trecv, tout, res,
    pos, place, order, tab,
    loc_sem, d_send, d_recv, s_send, s_recv, t_send, t_recv, o_send, o_recv, r_send, r_recv,
):
    rows = q_ref.shape[1]
    here = q_ref.shape[2] // HD
    share = here // 2
    part = rows // frames
    scale = HD ** (-0.5)
    f = lax.axis_index("frame")
    x = lax.axis_index("space")
    c = lax.axis_index("head")
    others_f = [lax.rem(f + d, frames) for d in range(1, frames)]
    others_x = [lax.rem(x + d, spaces) for d in range(1, spaces)]
    others_c = [lax.rem(c + d, cores) for d in range(1, cores)]
    side = f // (frames // 2)
    far_first = [
        lax.rem(f + (1 - side) * (frames - 1 - i) + side * (1 + i), frames)
        for i in range(frames - 1)
    ]

    def remote(src, dst, send, recv, **target):
        return pltpu.make_async_remote_copy(
            src_ref=src, dst_ref=dst, send_sem=send, recv_sem=recv,
            device_id=target, device_id_type=MESH,
        )

    def lanes(h):
        return pl.ds(pl.multiple_of(h * HD, HD), HD)

    sources = (k_ref, v_ref, q_ref)
    for n, src in enumerate(sources):
        def local_start(h, _):
            pltpu.make_async_copy(src.at[0, :, lanes(h)], full.at[n, h], loc_sem.at[n]).start()
            return 0

        lax.fori_loop(0, here, local_start, 0)

    barrier = pltpu.get_barrier_semaphore()
    for other in others_c:
        pl.semaphore_signal(barrier, inc=1, device_id={"head": other}, device_id_type=MESH)
    for other in others_x:
        pl.semaphore_signal(barrier, inc=1, device_id={"space": other}, device_id_type=MESH)
    for other in others_f:
        pl.semaphore_signal(barrier, inc=1, device_id={"frame": other}, device_id_type=MESH)

    count = jnp.int32(0)
    for h in range(here):
        count = count + prof_ref[h]
    first_space = (count >= share).astype(jnp.int32)
    main_count = jnp.maximum(count, here - count)
    for e in range(cores):
        main = first_space if e == 0 else 1 - first_space
        major = jnp.int32(0)
        minor = main_count
        for h in range(here):
            p = prof_ref[e * here + h]
            is_main = p * main + (1 - p) * (1 - main)
            slot = jnp.clip(is_main * major + (1 - is_main) * minor, 0, here - 1)
            major = major + is_main
            minor = minor + (1 - is_main)
            away = ((slot >= share) & (slot < main_count)).astype(jnp.int32)
            owner = away * (1 - e) + (1 - away) * e
            pos[e * here + h] = slot
            place[e * here + h] = owner * here + (1 - p) * share + slot - (slot >= share).astype(jnp.int32) * share

    def fill(slot, _):
        head = jnp.int32(0)
        for h in range(here):
            head = head + jnp.where(pos[c * here + h] == slot, h, 0)
        order[slot] = jnp.clip(head, 0, here - 1)
        return 0

    lax.fori_loop(0, here, fill, 0)

    for n in range(3):
        pltpu.make_async_copy(full.at[n], full.at[n], loc_sem.at[n]).wait()

    def arrange(slot, _):
        head = order[slot]
        for n in range(3):
            mine_first[slot, n] = full[n, head]
        return 0

    lax.fori_loop(0, here, arrange, 0)

    pl.semaphore_wait(barrier, len(others_c) + len(others_x) + len(others_f))

    partner = others_c[0]

    def core_copy(j):
        return remote(mine_first.at[share + j], theirs.at[j], d_send.at[j], d_recv.at[j], head=partner)

    def core_start(j, _):
        core_copy(j).start()
        return 0

    lax.fori_loop(0, share, core_start, 0)

    main_space = c * (1 - first_space) + (1 - c) * first_space
    my_rows = pl.ds(pl.multiple_of(x * rows, rows), rows)
    mine = pl.ds(pl.multiple_of(f * part, part), part)

    def window_copy(j, other):
        return remote(
            tsend.at[j, other], trecv.at[f, j], t_send.at[other, j], t_recv.at[f, j], frame=other
        )

    def space_copy(j, other):
        return remote(
            kv.at[j, :, my_rows], kv.at[j, :, my_rows], s_send.at[other, j], s_recv.at[x, j], space=other
        )

    def gather(j, _):
        core_copy(j).wait_recv()
        borrowed = share + j < main_count
        for n in range(3):
            head_main = mine_first[j, n]
            head_rest = jnp.where(borrowed, theirs[j, n], mine_first[share + j, n])
            block = jnp.where(main_space == 1, head_rest, head_main)
            for g in range(frames):
                tsend[j, g, n] = block[g * part:(g + 1) * part]
            block = jnp.where(main_space == 1, head_main, head_rest)
            if n < 2:
                kv[j, n, my_rows] = block
            else:
                squery[j] = block
        for other in far_first:
            window_copy(j, other).start()

        @pl.when(j > 0)
        def _():
            for other in others_x:
                space_copy(j - 1, other).start()

        return 0

    lax.fori_loop(0, share, gather, 0)

    def fill_reach(j, _):
        own_slot = j + main_space * share
        far = ((main_space == 1) & (share + j < main_count)).astype(jnp.int32)
        own_reach = jnp.int32(0)
        far_reach = jnp.int32(0)
        for h in range(here):
            own_reach = own_reach + jnp.where(pos[c * here + h] == own_slot, win_ref[c * here + h], 0)
            far_reach = far_reach + jnp.where(
                pos[partner * here + h] == share + j, win_ref[partner * here + h], 0
            )
        tab[j] = far * far_reach + (1 - far) * own_reach
        return 0

    lax.fori_loop(0, share, fill_reach, 0)

    def out_copy(j, other):
        return remote(
            tout.at[j, other], res.at[c * here + share + j, mine], o_send.at[other, j], o_recv.at[f, j], frame=other
        )

    def back_copy(slot, other):
        return remote(
            res.at[c * here + slot], res.at[c * here + slot], r_send.at[other, slot], r_recv.at[c, slot], head=other
        )

    for other in others_x:
        space_copy(share - 1, other).start()

    def step(j, _):
        for other in others_f:
            remote(
                tsend.at[j, other], trecv.at[other, j], t_send.at[other, j], t_recv.at[other, j], frame=other
            ).wait_recv()
        trecv[f, j] = tsend[j, f]
        reach = tab[j]
        qs = [trecv[g, j, 2].astype(jnp.float32) for g in range(frames)]
        ks = [trecv[g, j, 0].astype(jnp.float32) for g in range(frames)]
        vs = [trecv[g, j, 1].astype(jnp.float32) for g in range(frames)]
        for g in range(frames):
            near = [m for m in range(frames) if abs(m - g) <= WMAX]
            scores = []
            for m in near:
                raw = jnp.sum(qs[g] * ks[m], axis=-1, keepdims=True) * scale
                scores.append(jnp.where(reach >= abs(m - g), raw, -1e30))
            peak = functools.reduce(jnp.maximum, scores)
            weights = [jnp.exp(s - peak) for s in scores]
            total = functools.reduce(jnp.add, weights)
            acc = functools.reduce(
                jnp.add,
                [w.astype(jnp.bfloat16).astype(jnp.float32) * vs[m] for w, m in zip(weights, near)],
            )
            tout[j, g] = (acc / total).astype(jnp.bfloat16)
        res[c * here + share + j, mine] = tout[j, f]

        for other in others_x:
            other_rows = pl.ds(pl.multiple_of(other * rows, rows), rows)
            remote(
                kv.at[j, :, other_rows], kv.at[j, :, other_rows],
                s_send.at[other, j], s_recv.at[other, j], space=other,
            ).wait_recv()
        query = squery[j]
        scores = lax.dot_general(
            query, kv[j, 0], (((1,), (1,)), ((), ())), preferred_element_type=jnp.float32
        ) * scale
        peak = jnp.max(scores, axis=1, keepdims=True)
        weights = jnp.exp(scores - peak)
        total = jnp.sum(weights, axis=1, keepdims=True)
        acc = jnp.dot(weights.astype(jnp.bfloat16), kv[j, 1], preferred_element_type=jnp.float32)
        res[c * here + j] = (acc / total).astype(jnp.bfloat16)

        for other in far_first:
            out_copy(j, other).start()

        @pl.when(j > 0)
        def _():
            for other in others_c:
                back_copy(j - 1, other).start()

        return 0

    lax.fori_loop(0, share, step, 0)
    for other in others_c:
        back_copy(share - 1, other).start()

    def forward(j, _):
        for other in others_f:
            theirs = pl.ds(pl.multiple_of(other * part, part), part)
            remote(
                tout.at[j, other], res.at[c * here + share + j, theirs], o_send.at[other, j], o_recv.at[other, j],
                frame=other,
            ).wait_recv()
        for other in others_c:
            back_copy(share + j, other).start()
        return 0

    lax.fori_loop(0, share, forward, 0)

    def arrive(slot, _):
        for other in others_c:
            remote(
                res.at[c * here + slot], res.at[other * here + slot], r_send.at[other, slot], r_recv.at[other, slot], head=other
            ).wait_recv()
        return 0

    lax.fori_loop(0, 2 * share, arrive, 0)

    for i in range(here):
        out_ref[i] = res[place[c * here + i]]


    def drain(j, _):
        core_copy(j).wait_send()
        for other in others_f:
            window_copy(j, other).wait_send()
            out_copy(j, other).wait_send()
        for other in others_x:
            space_copy(j, other).wait_send()
        for other in others_c:
            back_copy(j, other).wait_send()
            back_copy(share + j, other).wait_send()
        return 0

    lax.fori_loop(0, share, drain, 0)


def direct_kernel(
    frames, spaces, cores, fulls, nears, tab, q_ref, k_ref, v_ref, res,
    full, kv, tsend, trecv, tout, nsend, nrecv,
    loc_sem, word, s_send, s_recv, t_send, t_recv, o_send, o_recv, n_send, n_recv,
):
    rows = q_ref.shape[1]
    here = q_ref.shape[2] // HD
    part = rows // frames
    scale = HD ** (-0.5)
    f = lax.axis_index("frame")
    x = lax.axis_index("space")
    c = lax.axis_index("head")
    side = f // (frames // 2)

    def each(lower, upper, body):
        def run(i, _):
            body(i)
            return 0

        lax.fori_loop(lower, upper, run, 0)

    def of_core(counts):
        total = jnp.int32(counts[0])
        for e in range(1, cores):
            total = jnp.where(c == e, jnp.int32(counts[e]), total)
        return total

    n_full = of_core(fulls)
    n_near = of_core(nears)
    n_time = n_full + n_near
    n_space = here - n_time

    def remote(src, dst, send, recv, **target):
        return pltpu.make_async_remote_copy(
            src_ref=src, dst_ref=dst, send_sem=send, recv_sem=recv,
            device_id=target, device_id_type=MESH,
        )

    def lanes(h):
        return pl.ds(pl.multiple_of(h * HD, HD), HD)

    def there(way, d):
        other = f + (2 * way - 1) * d
        return (other >= 0) & (other < frames)

    def away(way, d):
        return jnp.clip(f + (2 * way - 1) * d, 0, frames - 1)

    barrier = pltpu.get_barrier_semaphore()
    for d in range(1, spaces):
        pl.semaphore_signal(
            barrier, inc=1, device_id={"space": lax.rem(x + d, spaces)}, device_id_type=MESH
        )
    for way in range(2):
        @pl.when(there(way, 1))
        def _():
            pl.semaphore_signal(barrier, inc=1, device_id={"frame": away(way, 1)}, device_id_type=MESH)

    def all_in(view, sem):
        pltpu.make_async_copy(view, view, sem).wait()

    for n, src in enumerate((k_ref, v_ref, q_ref)):
        each(0, here, lambda h: pltpu.make_async_copy(
            src.at[0, :, lanes(h)], full.at[n, h], loc_sem.at[0]).start())
    all_in(full, loc_sem.at[0])

    pl.semaphore_wait(
        barrier, spaces - 1 + there(0, 1).astype(jnp.int32) + there(1, 1).astype(jnp.int32)
    )

    def tell(way, d):
        @pl.when(there(way, d) & there(1 - way, 1))
        def _():
            pl.semaphore_signal(
                word.at[way, d - 1], inc=1, device_id={"frame": away(1 - way, 1)}, device_id_type=MESH
            )

    if frames > 2:
        for way in range(2):
            tell(way, 1)

    my_rows = pl.ds(pl.multiple_of(x * rows, rows), rows)
    mine = pl.ds(pl.multiple_of(f * part, part), part)

    def window_copy(j, other):
        return remote(
            tsend.at[j, other], trecv.at[f, j], t_send.at[0], t_recv.at[j], frame=other
        )

    def space_copy(j, other):
        return remote(
            kv.at[j, :, my_rows], kv.at[j, :, my_rows], s_send.at[0], s_recv.at[j], space=other
        )

    def out_copy(j, other):
        return remote(
            tout.at[j, other], res.at[j, mine], o_send.at[0], o_recv.at[0], frame=other
        )

    def near_copy(j, way):
        return remote(
            nsend.at[j], nrecv.at[1 - way, j], n_send.at[way], n_recv.at[1 - way], frame=away(way, 1)
        )

    def other_spaces(body):
        each(1, spaces, lambda d: body(lax.rem(x + d, spaces)))

    def far_first(body):
        each(0, frames - 1, lambda i: body(
            lax.rem(f + (1 - side) * (frames - 1 - i) + side * (1 + i), frames)))

    def head_of(slot):
        return tab[slot]

    def send_at(j, d):
        def one(way):
            @pl.when(there(way, d))
            def _():
                window_copy(j, away(way, d)).start()

        each(0, 2, one)

    def prepare_space(j):
        head = head_of(n_time + j)
        for n in range(2):
            kv[j, n, my_rows] = full[n, head]
        other_spaces(lambda other: space_copy(j, other).start())

    def prepare(j):
        @pl.when(j < n_full)
        def _():
            head = head_of(j)
            for n in range(3):
                block = full[n, head]
                for g in range(frames):
                    tsend[j, g, n] = block[g * part:(g + 1) * part]
            send_at(j, 1)

        @pl.when(j == EARLY - 1)
        def _():
            each(0, n_space, prepare_space)
            for d in range(2, frames):
                for way in range(2):
                    @pl.when(there(way, d))
                    def _():
                        pl.semaphore_wait(word.at[way, d - 2], 1)

                    if d < frames - 1:
                        tell(way, d)

        @pl.when(j >= EARLY - 1)
        def _():
            each(2, frames, lambda i: send_at(j - EARLY + 1, frames + 1 - i))

    each(0, n_full + EARLY - 1, prepare)

    def prepare_near(j):
        head = head_of(n_full + j)
        for n in range(2):
            nsend[j, n] = full[n, head]

        def one(way):
            @pl.when(there(way, 1))
            def _():
                near_copy(j, way).start()

        each(0, 2, one)

    if max(nears) > 0:
        each(0, n_near, prepare_near)

    fine = min(part, 16)
    wide = min(rows, 128)

    def weigh(scores, values):
        peak = functools.reduce(jnp.maximum, scores)
        weights = [jnp.exp(s - peak) for s in scores]
        total = functools.reduce(jnp.add, weights)
        acc = functools.reduce(
            jnp.add,
            [w.astype(jnp.bfloat16).astype(jnp.float32) * v for w, v in zip(weights, values)],
        )
        return (acc / total).astype(jnp.bfloat16)

    def step(j):
        @pl.when(j < n_full)
        def _():
            all_in(trecv.at[pl.ds(0, frames - 1), j], t_recv.at[j])
            trecv[f, j] = tsend[j, f]
            reach = tab[2 * here + j]

            def rows_step(i):
                at = pl.ds(pl.multiple_of(i * fine, fine), fine)
                qs = [trecv[g, j, 2, at].astype(jnp.float32) for g in range(frames)]
                ks = [trecv[g, j, 0, at].astype(jnp.float32) for g in range(frames)]
                vs = [trecv[g, j, 1, at].astype(jnp.float32) for g in range(frames)]
                for g in range(frames):
                    close = [m for m in range(frames) if abs(m - g) <= WMAX]
                    scores = []
                    for m in close:
                        raw = jnp.sum(qs[g] * ks[m], axis=-1, keepdims=True) * scale
                        scores.append(jnp.where(reach >= abs(m - g), raw, -1e30))
                    tout[j, g, at] = weigh(scores, [vs[m] for m in close])

            each(0, part // fine, rows_step)
            res[j, mine] = tout[j, f]
            far_first(lambda other: out_copy(j, other).start())

        @pl.when(j < n_space)
        def _():
            all_in(kv.at[j, :, pl.ds(0, (spaces - 1) * rows)], s_recv.at[j])
            head = head_of(n_time + j)

            def query_step(i):
                at = pl.ds(pl.multiple_of(i * wide, wide), wide)
                scores = lax.dot_general(
                    full[2, head, at], kv[j, 0], (((1,), (1,)), ((), ())), preferred_element_type=jnp.float32
                ) * scale
                peak = jnp.max(scores, axis=1, keepdims=True)
                weights = jnp.exp(scores - peak)
                total = jnp.sum(weights, axis=1, keepdims=True)
                acc = jnp.dot(weights.astype(jnp.bfloat16), kv[j, 1], preferred_element_type=jnp.float32)
                res[n_time + j, at] = (acc / total).astype(jnp.bfloat16)

            each(0, rows // wide, query_step)

    each(0, here, step)

    def by_core(counts, body):
        for e in range(cores):
            if counts[e] > 0:
                @pl.when(c == e)
                def _():
                    body(counts[e])

    def near_arrivals(count):
        for way in range(2):
            @pl.when(there(way, 1))
            def _():
                all_in(nrecv.at[way, pl.ds(0, count)], n_recv.at[way])

            @pl.when(jnp.logical_not(there(way, 1)))
            def _():
                nrecv[way, pl.ds(0, count)] = nsend[pl.ds(0, count)]

    by_core(nears, near_arrivals)

    def near_step(j):
        head = head_of(n_full + j)

        def rows_step(i):
            at = pl.ds(pl.multiple_of(i * fine, fine), fine)
            query = full[2, head, at].astype(jnp.float32)
            keys = (nrecv[0, j, 0, at], nsend[j, 0, at], nrecv[1, j, 0, at])
            values = (nrecv[0, j, 1, at], nsend[j, 1, at], nrecv[1, j, 1, at])
            scores = []
            for key, take in zip(keys, (there(0, 1), None, there(1, 1))):
                raw = jnp.sum(query * key.astype(jnp.float32), axis=-1, keepdims=True) * scale
                scores.append(raw if take is None else jnp.where(take, raw, -1e30))
            res[n_full + j, at] = weigh(scores, [v.astype(jnp.float32) for v in values])

        each(0, rows // fine, rows_step)

    if max(nears) > 0:
        each(0, n_near, near_step)

    by_core(fulls, lambda count: all_in(res.at[pl.ds(0, count), pl.ds(0, rows - part)], o_recv.at[0]))


    def near_sent(count):
        for way in range(2):
            @pl.when(there(way, 1))
            def _():
                all_in(nsend.at[pl.ds(0, count)], n_send.at[way])

    by_core(fulls, lambda count: all_in(tsend.at[pl.ds(0, count), pl.ds(0, frames - 1)], t_send.at[0]))
    by_core(fulls, lambda count: all_in(tout.at[pl.ds(0, count), pl.ds(0, frames - 1)], o_send.at[0]))
    by_core(
        [here - t - n for t, n in zip(fulls, nears)],
        lambda count: [all_in(kv.at[pl.ds(0, count), :, pl.ds(0, rows)], s_send.at[0]) for _ in range(1, spaces)],
    )
    by_core(nears, near_sent)


def direct(sizes, times, nears, number, queries, key_states, value_states, profile, window, table):
    frames, spaces, cores = sizes
    rows = queries.shape[1]
    here = queries.shape[2] // HD
    part = rows // frames
    fulls = tuple(t - n for t, n in zip(times, nears))
    most_full, most_near = max(1, *fulls), max(1, *nears)
    most_space = max(1, *(here - t for t in times))
    bf = jnp.bfloat16
    dma = pltpu.SemaphoreType.DMA
    return pl.pallas_call(
        functools.partial(direct_kernel, frames, spaces, cores, fulls, nears),
        out_shape=pltpu.VMEM((here, rows, HD), queries.dtype),
        in_specs=[pl.BlockSpec(memory_space=pltpu.SMEM)] + [pl.BlockSpec(memory_space=pltpu.HBM)] * 3,
        out_specs=pl.BlockSpec(memory_space=pltpu.VMEM),
        scratch_shapes=[
            pltpu.VMEM((3, here, rows, HD), bf),
            pltpu.VMEM((most_space, 2, spaces * rows, HD), bf),
            pltpu.VMEM((most_full, frames, 3, part, HD), bf),
            pltpu.VMEM((frames, most_full, 3, part, HD), bf),
            pltpu.VMEM((most_full, frames, part, HD), bf),
            pltpu.VMEM((most_near, 2, rows, HD), bf),
            pltpu.VMEM((2, most_near, 2, rows, HD), bf),
            dma((1,)),
            pltpu.SemaphoreType.REGULAR((2, max(1, frames - 2))),
            dma((1,)),
            dma((most_space,)),
            dma((1,)),
            dma((most_full,)),
            dma((1,)),
            dma((1,)),
            dma((2,)),
            dma((2,)),
        ],
        compiler_params=pltpu.CompilerParams(
            collective_id=number, has_side_effects=True, vmem_limit_bytes=60 * 1024 * 1024
        ),
    )(table, queries, key_states, value_states)


def shared(sizes, queries, key_states, value_states, profile, window, table):
    frames, spaces, cores = sizes
    rows = queries.shape[1]
    here = queries.shape[2] // HD
    share = here // 2
    part = rows // frames
    any_space = pl.BlockSpec(memory_space=pltpu.HBM)
    bf = jnp.bfloat16
    dma = pltpu.SemaphoreType.DMA
    return pl.pallas_call(
        functools.partial(shared_kernel, frames, spaces, cores),
        out_shape=pltpu.VMEM((here, rows, HD), queries.dtype),
        in_specs=[pl.BlockSpec(memory_space=pltpu.SMEM)] * 2 + [any_space] * 3,
        out_specs=pl.BlockSpec(memory_space=pltpu.VMEM),
        scratch_shapes=[
            pltpu.VMEM((3, here, rows, HD), bf),
            pltpu.VMEM((here, 3, rows, HD), bf),
            pltpu.VMEM((share, 3, rows, HD), bf),
            pltpu.VMEM((share, rows, HD), bf),
            pltpu.VMEM((share, 2, spaces * rows, HD), bf),
            pltpu.VMEM((share, frames, 3, part, HD), bf),
            pltpu.VMEM((frames, share, 3, part, HD), bf),
            pltpu.VMEM((share, frames, part, HD), bf),
            pltpu.VMEM((cores * 2 * share, rows, HD), bf),
            pltpu.SMEM((here * cores,), jnp.int32),
            pltpu.SMEM((here * cores,), jnp.int32),
            pltpu.SMEM((here,), jnp.int32),
            pltpu.SMEM((share,), jnp.int32),
            dma((5,)),
            dma((share,)),
            dma((share,)),
            dma((spaces, share)),
            dma((spaces, share)),
            dma((frames, share)),
            dma((frames, share)),
            dma((frames, share)),
            dma((frames, share)),
            dma((cores, 2 * share)),
            dma((cores, 2 * share)),
        ],
        compiler_params=pltpu.CompilerParams(
            collective_id=0, has_side_effects=True, vmem_limit_bytes=60 * 1024 * 1024
        ),
    )(profile, window, queries, key_states, value_states)


def place_kernel(tab, res, out_ref, sem):
    here = res.shape[0]

    def put(slot, _):
        at = pl.ds(pl.multiple_of(tab[slot] * HD, HD), HD)
        pltpu.make_async_copy(res.at[slot], out_ref.at[0, :, at], sem.at[0]).start()
        return 0

    lax.fori_loop(0, here, put, 0)
    pltpu.make_async_copy(res, res, sem.at[0]).wait()


def choose_kernel(
    cores, caps, prof_ref, win_ref, out_ref, tab, prof_out, win_out
):
    here = prof_ref.shape[0] // cores
    c = lax.axis_index("head")
    first = jnp.int32(0)
    for h in range(here):
        first = first + 1 - prof_ref[h]
    nears = []
    for e in range(cores):
        near = jnp.int32(0)
        for h in range(e * here, (e + 1) * here):
            near = near + (1 - prof_ref[h]) * (win_ref[h] == 1).astype(jnp.int32)
        nears.append(near)
    index = jnp.int32(0)
    base = 1
    for count, most in caps.items():
        here_index = jnp.int32(0)
        size = 1
        for near, cap in zip(nears, most):
            here_index = here_index * (cap + 1) + jnp.minimum(near, cap)
            size = size * (cap + 1)
        index = jnp.where(first == count, base + here_index, index)
        base = base + size
    out_ref[0] = index

    kinds = []
    for h in range(here):
        p = prof_ref[c * here + h]
        kinds.append(p * 2 + (1 - p) * (win_ref[c * here + h] == 1).astype(jnp.int32))
    tops = [jnp.int32(0)]
    for kind in range(2):
        top = tops[-1]
        for h in range(here):
            top = top + (kinds[h] == kind).astype(jnp.int32)
        tops.append(top)
    for h in range(here):
        slot = jnp.where(kinds[h] == 0, tops[0], jnp.where(kinds[h] == 1, tops[1], tops[2]))
        for kind in range(3):
            tops[kind] = tops[kind] + (kinds[h] == kind).astype(jnp.int32)
        tab[slot] = h
        tab[here + h] = slot
        tab[2 * here + slot] = win_ref[c * here + h]
    @pl.when(index == 0)
    def _():
        for h in range(here):
            tab[h] = h

        def keep(h, _):
            prof_out[h] = prof_ref[h]
            win_out[h] = win_ref[h]
            return 0

        lax.fori_loop(0, here * cores, keep, 0)


def local(sizes, queries, key_states, value_states, profile, window):
    frames, spaces, cores = sizes
    here = queries.shape[2] // HD
    caps = {here // 2 + d: most for d, most in CAPS.items()}
    smem = pl.BlockSpec(memory_space=pltpu.SMEM)
    vmem = pl.BlockSpec(memory_space=pltpu.VMEM)
    hbm = pl.BlockSpec(memory_space=pltpu.HBM)
    index, table, profile, window = pl.pallas_call(
        functools.partial(choose_kernel, cores, caps),
        out_shape=(
            pltpu.SMEM((1,), jnp.int32),
            pltpu.SMEM((3 * here,), jnp.int32),
            pltpu.SMEM(profile.shape, profile.dtype),
            pltpu.SMEM(window.shape, window.dtype),
        ),
        in_specs=[smem, smem],
        out_specs=(smem, smem, smem, smem),
    )(profile, window)
    ways = [functools.partial(shared, sizes)]
    for first, most in caps.items():
        for nears in itertools.product(*(range(cap + 1) for cap in most)):
            ways.append(functools.partial(direct, sizes, (first, here - first), nears, len(ways)))
    result = lax.switch(index[0], ways, queries, key_states, value_states, profile, window, table)
    return pl.pallas_call(
        place_kernel,
        out_shape=jax.ShapeDtypeStruct(queries.shape, queries.dtype),
        in_specs=[smem, vmem],
        out_specs=hbm,
        scratch_shapes=[pltpu.SemaphoreType.DMA((1,))],
    )(table, result)


def solution(mesh):
    spec = P(("groups", "frame"), "space", "head")
    sizes = (mesh.shape["frame"], mesh.shape["space"], mesh.shape["head"])
    return jax.shard_map(
        functools.partial(local, sizes),
        mesh=mesh,
        in_specs=(spec, spec, spec, P(), P()),
        out_specs=spec,
        check_vma=False,
    )
```
